32 devices in a mesh: sector: 4 (over y, core), ops: 8 (over z, x).
Axes of the slice: x: 2, y: 2, z: 4, core: 2. Of those that a mesh axis runs over, the one named last changes fastest.
Arguments:
- wavefunction: bfloat16 [4, 1024, 1024], P('sector', 'ops'), may hold values from -6 to 6
- diag_scale: float32 [4, 1024, 1024], P('sector', 'ops'), may hold values from 1 to 8
- sector_dims: int32 [4], P('sector'), may hold values from 512 to 1024
- left_ops: bfloat16 [4, 16, 1024, 1024], P('sector', 'ops'), may hold values from -0.1875 to 0.1875
- right_ops: bfloat16 [4, 16, 1024, 1024], P('sector', 'ops'), may hold values from -0.1875 to 0.1875
- weight_index: int32 [4, 16], P('sector', 'ops'), may hold values from 0 to 15
- weight_table: float32 [16], replicated, may hold values from -1 to 1
Outputs:
- basis: bfloat16 [4, 1024, 1024], P('sector', 'ops')
- energy: float32 [4], P('sector')
- next_ops: float32 [1024, 1024], P('ops')
The draws below stay inside these ranges and needn't reach their ends.
All inputs are finite; a program needn't handle non-finite values.
Results may differ from the reference program's by a relative error of at most 0.025.
Values may be sent and summed in bfloat16 or wider, within the bound.
A program may use at most 128 MiB of HBM per device.

```python
import math
import jax
import jax.numpy as jnp
from jax import lax

K = 1024
KEEP = 1024
NW = 16
GROUPS = 4
PAIRS = 16


def set_ends(entries, stream_key, smallest, largest):
    spot = [jax.random.randint(jax.random.fold_in(stream_key, axis), (), 0, length) for axis, length in enumerate(entries.shape)]
    main_axis = entries.shape.index(max(entries.shape))
    neighbour = spot[:main_axis] + [(spot[main_axis] + 1) % entries.shape[main_axis]] + spot[main_axis + 1:]
    return entries.at[tuple(spot)].set(smallest).at[tuple(neighbour)].set(largest)


def block_levels(own_key, shape, shards, low, high):
    level = 1.0
    for axis_at, parts in shards:
        heights = jax.random.uniform(jax.random.fold_in(jax.random.fold_in(own_key, 6), axis_at), (parts,), jnp.float32, low / len(shards), high / len(shards))
        level = level * jnp.repeat(jnp.exp(heights), shape[axis_at] // parts).reshape((-1,) + (1,) * (len(shape) - 1 - axis_at))
    return level


def bell_draw(stream_key, shape, deviation, most, pieces=(), held_as=jnp.bfloat16):
    values = deviation * jax.random.normal(stream_key, shape, jnp.float32)
    if pieces:
        values = values * block_levels(stream_key, shape, pieces, -0.22, 0.18)
    return jnp.clip(values, -most, most).astype(held_as)


def setup_inputs(seed: int = 0) -> dict:
    arg_keys = jax.random.split(jax.random.key(seed), 8)
    return {
        "wavefunction": bell_draw(arg_keys[0], (GROUPS, K, K), 1.0, 6.0, ((0, 4), (1, 8))),
        "diag_scale": jnp.clip(jnp.exp(math.log(8.0) - 2.0794415 * jax.random.uniform(arg_keys[1], (GROUPS, K, K), jnp.float32) ** block_levels(arg_keys[1], (GROUPS, K, K), ((0, 4), (1, 8)), -0.2, 0.2)), 1.0, 8.0),
        "sector_dims": set_ends(jax.random.randint(arg_keys[2], (GROUPS,), K // 2, K + 1), jax.random.fold_in(arg_keys[2], 1), K // 2, K).astype(jnp.int32),
        "left_ops": bell_draw(arg_keys[3], (GROUPS, PAIRS, K, K), K ** -0.5, 0.1875, ((0, 4), (1, 8))),
        "right_ops": bell_draw(arg_keys[4], (GROUPS, PAIRS, K, K), K ** -0.5, 0.1875, ((0, 4), (1, 8))),
        "weight_index": set_ends(jax.random.randint(arg_keys[5], (GROUPS, PAIRS), 0, NW), jax.random.fold_in(arg_keys[5], 1), 0, NW - 1).astype(jnp.int32),
        "weight_table": jnp.clip(jax.random.uniform(arg_keys[6], (NW,), jnp.float32, -1.0, 1.0), -1.0, 1.0),
    }


def group_step(psi, scale, dim, left, right, index, table):
    order_k = psi.shape[0]
    rows = jnp.arange(order_k)
    live = rows < dim
    mask = live[:, None] & live[None, :]
    psi_m = jnp.where(mask, psi, jnp.zeros_like(psi))
    onehot = (index[:, None] == jnp.arange(table.shape[0])[None, :]).astype(jnp.float32)
    coef = jnp.sum(onehot * table[None, :], axis=1)

    def add_pair(total, item):
        left_p, right_p, weight = item
        applied = jnp.dot(left_p.astype(jnp.float32), psi_m.astype(jnp.float32), preferred_element_type=jnp.float32).astype(jnp.bfloat16)
        term = lax.dot_general(applied.astype(jnp.float32), right_p.astype(jnp.float32), (((1,), (1,)), ((), ())), preferred_element_type=jnp.float32)
        return (total + weight * term, None)
    sigma, _ = lax.scan(add_pair, jnp.zeros((order_k, order_k), jnp.float32), (left, right, coef))
    sigma = jnp.where(mask, sigma, jnp.float32(0.0))
    psi_f = psi_m.astype(jnp.float32)
    energy = jnp.sum(psi_f * sigma) / jnp.sum(psi_f * psi_f)
    update = psi_f + (sigma - energy * psi_f) / scale
    columns = update[:, :KEEP]
    gram = jnp.dot(columns.T, columns, precision=lax.Precision.HIGHEST) / order_k
    gram = gram + 0.001 * jnp.eye(KEEP, dtype=jnp.float32)
    factor = jnp.linalg.cholesky(gram)
    basis = jax.scipy.linalg.solve_triangular(factor, columns.T, lower=True).T.astype(jnp.bfloat16)

    def rotate_pair(total, item):
        left_p, weight = item
        moved = jnp.dot(left_p.astype(jnp.float32), basis.astype(jnp.float32), preferred_element_type=jnp.float32).astype(jnp.bfloat16)
        rotated = jnp.dot(basis.T.astype(jnp.float32), moved.astype(jnp.float32), preferred_element_type=jnp.float32) / order_k
        return (total + weight * rotated, None)
    summed, _ = lax.scan(rotate_pair, jnp.zeros((KEEP, KEEP), jnp.float32), (left, coef))
    return (basis, energy, summed)

def reference(wavefunction, diag_scale, sector_dims, left_ops, right_ops, weight_index, weight_table):

    def one_group(items):
        psi, scale, dim, left, right, index = items
        return group_step(psi, scale, dim, left, right, index, weight_table)
    basis, energy, summed = lax.map(one_group, (wavefunction, diag_scale, sector_dims, left_ops, right_ops, weight_index))
    return (basis, energy, jnp.sum(summed, axis=0))
```

```python
import functools

import jax
import jax.numpy as jnp
from jax import lax
from jax.experimental import pallas as pl
from jax.experimental.pallas import tpu as pltpu
from jax.sharding import PartitionSpec as P

BLOCK = 128
SUB = 8
MESH = pl.DeviceIdType.MESH
VMEM_LIMIT = 60 * 2**20
F32 = jnp.float32
BF16 = jnp.bfloat16


def split3(u):
    high = u.astype(jnp.bfloat16).astype(jnp.float32)
    rest = u - high
    mid = rest.astype(jnp.bfloat16).astype(jnp.float32)
    low = (rest - mid).astype(jnp.bfloat16).astype(jnp.float32)
    return high, mid, low


def inverse_factor(block):
    size = block.shape[0]
    lane = lax.broadcasted_iota(jnp.int32, (SUB, size), 1)
    row = lax.broadcasted_iota(jnp.int32, (SUB, size), 0)
    below = block
    done = []
    for s in range(size // SUB):
        at = s * SUB
        top = below[:SUB]
        columns = [
            jnp.broadcast_to(top[:, at + j : at + j + 1], (SUB, size)) for j in range(SUB)
        ]
        here = (lane >= at) & (lane < at + SUB)
        body = jnp.where(here, (lane - at == row).astype(jnp.float32), top)
        pivots = jnp.ones((SUB, size), jnp.float32)
        for j in range(SUB):
            pivot = jnp.broadcast_to(columns[j][j : j + 1], (SUB, size))
            pivots = jnp.where(row == j, pivot, pivots)
            if j < SUB - 1:
                factor = jnp.where(row > j, columns[j] / pivot, 0.0)
                for c in range(j + 1, SUB):
                    columns[c] = columns[c] - factor * columns[c][j : j + 1]
                body = body - factor * body[j : j + 1]
        scaled = body * lax.rsqrt(pivots)
        done.append(scaled)
        if at + SUB < size:
            high, mid, low = split3(scaled)
            left = jnp.concatenate([high, high, mid, high, mid, low], axis=0)
            right = jnp.concatenate([high, mid, high, low, mid, high], axis=0)
            outer = lax.dot_general(
                left.T.astype(jnp.bfloat16),
                right.astype(jnp.bfloat16),
                (((1,), (0,)), ((), ())),
                preferred_element_type=jnp.float32,
            )
            rows_left = size - at - SUB
            lanes = lax.broadcasted_iota(jnp.int32, (rows_left, size), 1)
            kept = jnp.where((lanes >= at) & (lanes < at + SUB), 0.0, below[SUB:])
            below = kept - outer[at + SUB :]
    whole = jnp.concatenate(done, axis=0)
    r = lax.broadcasted_iota(jnp.int32, (size, size), 0)
    c = lax.broadcasted_iota(jnp.int32, (size, size), 1)
    return jnp.where(c <= r, whole, 0.0)


def place(owners):
    me = lax.axis_index("ops")
    return me, me // 2, lax.rem(me, 2)


def send(src, dst, send_sem, recv_sem, target, axis="ops"):
    return pltpu.make_async_remote_copy(
        src_ref=src,
        dst_ref=dst,
        send_sem=send_sem,
        recv_sem=recv_sem,
        device_id={axis: target},
        device_id_type=MESH,
    )


def greet(owners):
    me, pair, side = place(owners)
    half = owners // 2
    barrier = pltpu.get_barrier_semaphore()
    pl.semaphore_signal(
        barrier, inc=1, device_id={"ops": pair * 2 + 1 - side}, device_id_type=MESH
    )
    for k in range(1, half):
        pl.semaphore_signal(
            barrier,
            inc=1,
            device_id={"ops": lax.rem(pair + k, half) * 2 + side},
            device_id_type=MESH,
        )
    pl.semaphore_wait(barrier, half)


def gather_start(owners, own, blocks, send_sem, recv_sem):
    me, pair, side = place(owners)
    half = owners // 2
    for k in range(1, half):
        target = lax.rem(pair + k, half) * 2 + side
        send(own, blocks.at[me], send_sem.at[k], recv_sem.at[me], target).start()
    send(own, blocks.at[me], send_sem.at[0], recv_sem.at[me], pair * 2 + 1 - side).start()


def gather_receive(owners, own, blocks, send_sem, recv_sem, source):
    me, pair, side = place(owners)
    send(own, blocks.at[source], send_sem.at[0], recv_sem.at[source], me).wait_recv()


def gather_pass_on(owners, k, own, blocks, send_sem, recv_sem):
    me, pair, side = place(owners)
    half = owners // 2
    source = lax.rem(pair - k + half, half) * 2 + side
    gather_receive(owners, own, blocks, send_sem, recv_sem, source)
    send(
        blocks.at[source],
        blocks.at[source],
        send_sem.at[half - 1 + k],
        recv_sem.at[source],
        pair * 2 + 1 - side,
    ).start()
    return source


def gather_partner(owners, k, own, blocks, send_sem, recv_sem):
    me, pair, side = place(owners)
    half = owners // 2
    source = lax.rem(pair - k + half, half) * 2 + 1 - side
    gather_receive(owners, own, blocks, send_sem, recv_sem, source)
    return source


def gather_finish(owners, own, blocks, send_sem, recv_sem):
    me, pair, side = place(owners)
    for k in range(owners - 1):
        send(own, blocks.at[me], send_sem.at[k], recv_sem.at[me], me).wait_send()


def sigma_kernel(
    owners,
    psi_ref,
    diag_ref,
    dim_ref,
    index_ref,
    table_ref,
    left_hbm,
    right_hbm,
    columns_hbm,
    gram_ref,
    energy_ref,
    operator_ref,
    left,
    right,
    psi_all,
    psi_live,
    turned,
    sums,
    pair_out,
    pair_in,
    cross_out,
    cross_in,
    number,
    own,
    columns,
    load_sem,
    a_send,
    a_recv,
    p_send,
    p_recv,
    c_send,
    c_recv,
    n_send,
    n_recv,
    x_send,
    x_recv,
    store_sem,
):
    me, pair, side = place(owners)
    half = owners // 2
    partner = pair * 2 + 1 - side
    rows, order = psi_ref.shape
    pairs = left.shape[0]
    dim = dim_ref[0]
    coef = [table_ref[index_ref[0, p]] for p in range(pairs)]

    loads = [pltpu.make_async_copy(right_hbm.at[0], right, load_sem.at[0])]
    loads.append(pltpu.make_async_copy(left_hbm.at[0], left, load_sem.at[1]))
    for load in loads:
        load.start()
    greet(owners)
    gather = (owners, psi_ref, psi_all, a_send, a_recv)
    gather_start(*gather)

    lane = lax.broadcasted_iota(jnp.int32, (rows, order), 1)
    row = lax.broadcasted_iota(jnp.int32, (rows, order), 0)

    def masked(block, owner):
        return jnp.where((lane < dim) & (row + owner * rows < dim), block, jnp.zeros_like(block))

    def turn(block, owner):
        live = masked(block, owner)
        psi_live[owner] = live
        for p in range(pairs):
            turned[p, pl.ds(pl.multiple_of(owner * rows, rows), rows), :] = (
                coef[p]
                * lax.dot_general(
                    live, right[p], (((1,), (1,)), ((), ())), preferred_element_type=F32
                )
            ).astype(BF16)

    loads[0].wait()
    turn(psi_ref[...], me)

    def arrive(k, carry):
        source = gather_pass_on(owners, k, *gather[1:])
        turn(psi_all[source], source)
        source = gather_partner(owners, k - 1, *gather[1:])
        turn(psi_all[source], source)
        return carry

    lax.fori_loop(1, half, arrive, 0)
    source = gather_partner(owners, half - 1, *gather[1:])
    turn(psi_all[source], source)
    loads[1].wait()

    def partial(k, numer):
        at = lax.rem(pair + k, half)
        here = pl.ds(pl.multiple_of(at * 2 * rows, 2 * rows), 2 * rows)
        total = jnp.dot(left[0, here, :], turned[0], preferred_element_type=F32)
        for p in range(1, pairs):
            total += jnp.dot(left[p, here, :], turned[p], preferred_element_type=F32)
        sums[k - 1] = total.reshape(2, rows, order)
        pair_out[k - 1] = sums[k - 1, 1 - side].astype(BF16)
        send(
            pair_out.at[k - 1],
            pair_in.at[k - 1],
            p_send.at[k - 1],
            p_recv.at[k - 1],
            partner,
        ).start()
        for j in range(2):
            product = psi_live[at * 2 + j].astype(F32) * sums[k - 1, j]
            numer = numer + jnp.sum(product.reshape(rows // 8, 8, order), axis=0)
        return numer

    numer = lax.fori_loop(1, half + 1, partial, jnp.zeros((8, order), F32))
    number[0] = jnp.full((8, 128), jnp.sum(numer), F32)
    send(number.at[0], number.at[1], n_send.at[0], n_recv.at[0], partner).start()

    def operate(i, carry):
        here = pl.ds(pl.multiple_of(i * 128, 128), 128)
        total = coef[0] * left[0, here, :].astype(F32)
        for p in range(1, pairs):
            total += coef[p] * left[p, here, :].astype(F32)
        operator_ref[here, :] = total.astype(BF16)
        return carry

    lax.fori_loop(0, order // 128, operate, 0)

    def square(i, carry):
        live = psi_live[i].astype(F32)
        return carry + jnp.sum((live * live).reshape(rows // 8, 8, order), axis=0)

    denom = jnp.sum(lax.fori_loop(0, owners, square, jnp.zeros((8, order), F32)))

    send(number.at[0], number.at[1], n_send.at[0], n_recv.at[0], partner).wait_recv()
    number[2 + pair] = number[0] + number[1]
    for k in range(1, half):
        send(
            number.at[2 + pair],
            number.at[2 + pair],
            n_send.at[k],
            n_recv.at[1 + pair],
            lax.rem(pair + k, half) * 2 + side,
        ).start()

    def crossing(k):
        return send(
            cross_out.at[k - 1],
            cross_in.at[k - 1],
            c_send.at[k - 1],
            c_recv.at[k - 1],
            lax.rem(pair + k, half) * 2 + side,
        )

    def pairing(k):
        return send(
            pair_out.at[k - 1], pair_in.at[k - 1], p_send.at[k - 1], p_recv.at[k - 1], partner
        )

    def cross(k, carry):
        pairing(k).wait_recv()
        cross_out[k - 1] = (sums[k - 1, side] + pair_in[k - 1].astype(F32)).astype(BF16)
        crossing(k).start()
        return carry

    lax.fori_loop(1, half, cross, 0)
    for k in range(1, half):
        source = lax.rem(pair + k, half)
        send(
            number.at[2 + pair], number.at[2 + source], n_send.at[k], n_recv.at[1 + source], me
        ).wait_recv()
    energy = number[2]
    for i in range(1, half):
        energy = energy + number[2 + i]
    energy = energy / denom
    energy_ref[...] = energy
    energy = jnp.max(energy)

    pairing(half).wait_recv()
    total = sums[half - 1, side] + pair_in[half - 1].astype(F32)
    sums[half - 1, side] = total

    def take(k, carry):
        crossing(k).wait_recv()
        sums[half - 1, side] += cross_in[k - 1].astype(F32)
        return carry

    lax.fori_loop(1, half, take, 0)
    sigma = masked(sums[half - 1, side], me)
    psi = psi_live[me].astype(F32)
    own[...] = (psi + (sigma - energy * psi) / diag_ref[...]).astype(BF16)
    gather = (owners, own, columns, x_send, x_recv)
    gather_start(*gather)

    step = 256

    def square_up(block, first):
        for i in range(0, order, step):
            part = lax.dot_general(
                block[:, i : i + step],
                block[:, i:],
                (((0,), (0,)), ((), ())),
                preferred_element_type=F32,
            )
            if first:
                gram_ref[i : i + step, i:] = part
            else:
                gram_ref[i : i + step, i:] += part

    columns[me] = own[...]
    square_up(own[...], True)

    def meet(k, carry):
        one = gather_pass_on(owners, k, *gather[1:])
        two = gather_partner(owners, k - 1, *gather[1:])
        square_up(jnp.concatenate([columns[one], columns[two]], axis=0), False)
        return carry

    lax.fori_loop(1, half, meet, 0)
    last = gather_partner(owners, half - 1, *gather[1:])
    store = pltpu.make_async_copy(columns, columns_hbm, store_sem.at[0])
    store.start()
    square_up(columns[last], False)

    gather_finish(*gather)
    gather_finish(owners, psi_ref, psi_all, a_send, a_recv)
    for k in range(1, half + 1):
        pairing(k).wait_send()
    for k in range(1, half):
        crossing(k).wait_send()
    for k in range(half):
        send(number.at[0], number.at[1], n_send.at[k], n_recv.at[0], partner).wait_send()
    store.wait()


def sigma_stage(psi, diag, dim, left, right, index, table):
    owners = lax.axis_size("ops")
    half = owners // 2
    rows, order = psi.shape
    pairs = left.shape[1]
    vmem = pl.BlockSpec(memory_space=pltpu.VMEM)
    smem = pl.BlockSpec(memory_space=pltpu.SMEM)
    hbm = pl.BlockSpec(memory_space=pl.ANY)
    dma = pltpu.SemaphoreType.DMA
    return pl.pallas_call(
        functools.partial(sigma_kernel, owners),
        out_shape=(
            jax.ShapeDtypeStruct((owners, rows, order), BF16),
            jax.ShapeDtypeStruct((order, order), F32),
            jax.ShapeDtypeStruct((8, 128), F32),
            jax.ShapeDtypeStruct((order, order), BF16),
        ),
        in_specs=[vmem, vmem, smem, smem, smem, hbm, hbm],
        out_specs=(hbm, vmem, vmem, vmem),
        scratch_shapes=[
            pltpu.VMEM((pairs, order, order), BF16),
            pltpu.VMEM((pairs, order, order), BF16),
            pltpu.VMEM((owners, rows, order), BF16),
            pltpu.VMEM((owners, rows, order), BF16),
            pltpu.VMEM((pairs, order, order), BF16),
            pltpu.VMEM((half, 2, rows, order), F32),
            pltpu.VMEM((half, rows, order), BF16),
            pltpu.VMEM((half, rows, order), BF16),
            pltpu.VMEM((half, rows, order), BF16),
            pltpu.VMEM((half, rows, order), BF16),
            pltpu.VMEM((2 + half, 8, 128), F32),
            pltpu.VMEM((rows, order), BF16),
            pltpu.VMEM((owners, rows, order), BF16),
            dma((2,)),
            dma((owners,)),
            dma((owners,)),
            dma((half,)),
            dma((half,)),
            dma((half,)),
            dma((half,)),
            dma((half,)),
            dma((half + 1,)),
            dma((owners,)),
            dma((owners,)),
            dma((1,)),
        ],
        compiler_params=pltpu.CompilerParams(
            collective_id=0, has_side_effects=True, vmem_limit_bytes=VMEM_LIMIT
        ),
        cost_estimate=pl.CostEstimate(
            flops=10 * order**3, bytes_accessed=20 * order**2, transcendentals=0
        ),
        name="sigma_stage",
    )(psi, diag, dim, index, table, left, right)


def inverse_kernel(
    owners,
    scale,
    gram_ref,
    operator_ref,
    high_ref,
    low_ref,
    whole_hbm,
    work,
    pair_in,
    cross_out,
    cross_in,
    own,
    whole,
    p_send,
    p_recv,
    c_send,
    c_recv,
    g_send,
    g_recv,
    store_sem,
):
    me, pair, side = place(owners)
    half = owners // 2
    partner = pair * 2 + 1 - side
    order = gram_ref.shape[0]
    blocks = order // BLOCK
    column = lax.broadcasted_iota(jnp.int32, (BLOCK, order), 1)
    local = lax.broadcasted_iota(jnp.int32, (BLOCK, order), 0)

    def pairing(k):
        return send(
            operator_ref.at[lax.rem(pair + k, half) * 2 + 1 - side],
            pair_in.at[k - 1],
            p_send.at[k - 1],
            p_recv.at[k - 1],
            partner,
        )

    def crossing(k):
        return send(
            cross_out.at[k - 1],
            cross_in.at[k - 1],
            c_send.at[k - 1],
            c_recv.at[k - 1],
            lax.rem(pair + k, half) * 2 + side,
        )

    gather = (owners, own, whole, g_send, g_recv)

    greet(owners)
    for k in range(1, half + 1):
        pairing(k).start()

    def cross():
        def one(k, carry):
            pairing(k).wait_recv()
            at = lax.rem(pair + k, half) * 2 + side
            cross_out[k - 1] = (
                operator_ref[at].astype(F32) + pair_in[k - 1].astype(F32)
            ).astype(BF16)

            @pl.when(k < half)
            def _():
                crossing(k).start()

            return carry

        lax.fori_loop(1, half + 1, one, 0)

    def settle():
        total = cross_out[half - 1].astype(F32)
        for k in range(1, half):
            crossing(k).wait_recv()
            total = total + cross_in[k - 1].astype(F32)
        own[...] = total.astype(BF16)
        gather_start(*gather)
        whole[me] = own[...]

    def hand_on():
        def one(k, carry):
            gather_pass_on(owners, k, *gather[1:])
            return carry

        lax.fori_loop(1, half, one, 0)

    def rows(i):
        return pl.ds(pl.multiple_of(i * BLOCK, BLOCK), BLOCK)

    def load(i, carry):
        eye = (column == local + i * BLOCK).astype(F32)
        work[rows(i), :] = gram_ref[rows(i), :] * scale + 0.001 * eye
        return carry

    lax.fori_loop(0, blocks, load, 0)

    def step(k, carry):
        first = k * BLOCK
        inverse = inverse_factor(work[rows(k), rows(k)])
        in_k = (column >= first) & (column < first + BLOCK)
        pivot_rows = jnp.where(in_k, (column - first == local).astype(F32), work[rows(k), :])
        work[rows(k), :] = jnp.dot(
            inverse, pivot_rows, precision=lax.Precision.HIGHEST, preferred_element_type=F32
        )

        def update(i, inner):
            panel = work[rows(k), rows(i)].T
            kept = jnp.where(in_k, 0.0, work[rows(i), :])
            work[rows(i), :] = kept - jnp.dot(
                panel,
                work[rows(k), :],
                precision=lax.Precision.HIGHEST,
                preferred_element_type=F32,
            )
            return inner

        lax.fori_loop(k + 1, blocks, update, 0)
        pl.when(k == blocks // 4)(cross)
        pl.when(k == blocks // 2)(settle)
        pl.when(k == blocks - 2)(hand_on)
        return carry

    lax.fori_loop(0, blocks, step, 0)

    def receive(k, carry):
        gather_partner(owners, k, *gather[1:])
        return carry

    lax.fori_loop(0, half, receive, 0)
    store_whole = pltpu.make_async_copy(whole, whole_hbm, store_sem.at[0])
    store_whole.start()

    def store(i, carry):
        kept = jnp.where(column <= local + i * BLOCK, work[rows(i), :], 0.0)
        high = kept.astype(BF16)
        high_ref[rows(i), :] = high
        low_ref[rows(i), :] = (kept - high.astype(F32)).astype(BF16)
        return carry

    lax.fori_loop(0, blocks, store, 0)
    gather_finish(*gather)
    for k in range(1, half + 1):
        pairing(k).wait_send()
    for k in range(1, half):
        crossing(k).wait_send()
    store_whole.wait()


def inverse_stage(gram, operator, scale):
    owners = lax.axis_size("ops")
    half_count = owners // 2
    order = gram.shape[0]
    rows = order // owners
    half = jax.ShapeDtypeStruct((order, order), BF16)
    vmem = pl.BlockSpec(memory_space=pltpu.VMEM)
    dma = pltpu.SemaphoreType.DMA
    operator = operator.reshape(owners, rows, order)
    return pl.pallas_call(
        functools.partial(inverse_kernel, owners, scale),
        out_shape=(half, half, jax.ShapeDtypeStruct((owners, rows, order), BF16)),
        in_specs=[vmem, vmem],
        out_specs=(vmem, vmem, pl.BlockSpec(memory_space=pl.ANY)),
        scratch_shapes=[
            pltpu.VMEM((order, order), F32),
            pltpu.VMEM((half_count, rows, order), BF16),
            pltpu.VMEM((half_count, rows, order), BF16),
            pltpu.VMEM((half_count, rows, order), BF16),
            pltpu.VMEM((rows, order), BF16),
            pltpu.VMEM((owners, rows, order), BF16),
            dma((half_count,)),
            dma((half_count,)),
            dma((half_count,)),
            dma((half_count,)),
            dma((owners,)),
            dma((owners,)),
            dma((1,)),
        ],
        compiler_params=pltpu.CompilerParams(
            collective_id=1, has_side_effects=True, vmem_limit_bytes=40 * 2**20
        ),
        cost_estimate=pl.CostEstimate(
            flops=400 * order**3 // 10, bytes_accessed=8 * order**2, transcendentals=0
        ),
        name="inverse_stage",
    )(gram, operator)


def sum_kernel(
    sectors, mine_ref, out_ref, one_out, one_in, two_out, two_in, three_in, sem_send, sem_recv
):
    me = lax.axis_index("sector")
    core = lax.rem(me, 2)
    chip = me // 2
    chips = sectors // 2
    partner = chip * 2 + 1 - core
    rows, order = mine_ref.shape
    part = rows // 2
    barrier = pltpu.get_barrier_semaphore()
    pl.semaphore_signal(barrier, inc=1, device_id={"sector": partner}, device_id_type=MESH)
    for k in range(1, chips):
        pl.semaphore_signal(
            barrier,
            inc=1,
            device_id={"sector": lax.rem(chip + k, chips) * 2 + core},
            device_id_type=MESH,
        )
    pl.semaphore_wait(barrier, chips)

    kept = pl.ds(pl.multiple_of(core * part, part), part)
    given = pl.ds(pl.multiple_of((1 - core) * part, part), part)
    one_out[...] = mine_ref[given, :].astype(BF16)
    first = send(one_out, one_in, sem_send.at[0], sem_recv.at[0], partner, "sector")
    first.start()
    first.wait_recv()
    two_out[...] = (mine_ref[kept, :] + one_in[...].astype(F32)).astype(BF16)
    for k in range(1, chips):
        send(
            two_out,
            two_in.at[chip],
            sem_send.at[k],
            sem_recv.at[1 + chip],
            lax.rem(chip + k, chips) * 2 + core,
            "sector",
        ).start()
    two_in[chip] = two_out[...]
    for k in range(1, chips):
        source = lax.rem(chip + k, chips)
        send(
            two_out, two_in.at[source], sem_send.at[k], sem_recv.at[1 + source], me, "sector"
        ).wait_recv()
    total = two_in[0].astype(F32)
    for i in range(1, chips):
        total = total + two_in[i].astype(F32)
    two_in[0] = total.astype(BF16)
    last = send(two_in.at[0], three_in, sem_send.at[chips], sem_recv.at[chips + 1], partner, "sector")
    last.start()
    out_ref[kept, :] = two_in[0].astype(F32)
    last.wait_recv()
    out_ref[given, :] = three_in[...].astype(F32)
    first.wait_send()
    for k in range(1, chips):
        send(
            two_out, two_in.at[chip], sem_send.at[k], sem_recv.at[1 + chip], me, "sector"
        ).wait_send()
    last.wait_send()


def sum_stage(mine):
    sectors = lax.axis_size("sector")
    chips = sectors // 2
    rows, order = mine.shape
    part = rows // 2
    vmem = pl.BlockSpec(memory_space=pltpu.VMEM)
    dma = pltpu.SemaphoreType.DMA
    return pl.pallas_call(
        functools.partial(sum_kernel, sectors),
        out_shape=jax.ShapeDtypeStruct((rows, order), F32),
        in_specs=[vmem],
        out_specs=vmem,
        scratch_shapes=[
            pltpu.VMEM((part, order), BF16),
            pltpu.VMEM((part, order), BF16),
            pltpu.VMEM((part, order), BF16),
            pltpu.VMEM((chips, part, order), BF16),
            pltpu.VMEM((part, order), BF16),
            dma((chips + 1,)),
            dma((chips + 2,)),
        ],
        compiler_params=pltpu.CompilerParams(collective_id=2, has_side_effects=True),
        cost_estimate=pl.CostEstimate(
            flops=order**2, bytes_accessed=4 * order**2, transcendentals=0
        ),
        name="sum_stage",
    )(mine)


def shards(wavefunction, diag_scale, sector_dims, left_ops, right_ops, weight_index, weight_table):
    rows_dev, order_k = wavefunction.shape[1:]
    first_row = lax.axis_index("ops") * rows_dev
    columns, product, energy, operator = sigma_stage(
        wavefunction[0],
        diag_scale[0],
        sector_dims,
        left_ops,
        right_ops,
        weight_index,
        weight_table,
    )
    high, low, operator = inverse_stage(product, operator, 1.0 / order_k)
    columns = columns.reshape(order_k, order_k)
    operator = operator.reshape(order_k, order_k)
    across = (((1,), (1,)), ((), ()))
    basis = (
        lax.dot_general(columns, high, across, preferred_element_type=F32)
        + lax.dot_general(columns, low, across, preferred_element_type=F32)
    ).astype(BF16)
    basis_local = lax.dynamic_slice_in_dim(basis, first_row, rows_dev, axis=0)
    own = lax.dynamic_slice_in_dim(basis, first_row, rows_dev, axis=1)
    half = lax.dot_general(
        own, operator, (((0,), (0,)), ((), ())), preferred_element_type=F32
    ).astype(BF16)
    rotated = jnp.dot(half, basis, preferred_element_type=F32) / order_k
    next_rows = sum_stage(rotated)
    return (basis_local[None], energy[0, :1], next_rows)


def solution(mesh):
    in_specs = (
        P("sector", "ops", None),
        P("sector", "ops", None),
        P("sector"),
        P("sector", "ops", None, None),
        P("sector", "ops", None, None),
        P("sector", "ops"),
        P(),
    )
    out_specs = (P("sector", "ops", None), P("sector"), P("ops", None))
    return jax.shard_map(shards, mesh=mesh, in_specs=in_specs, out_specs=out_specs, check_vma=False)
```

```python
import functools

import jax
import jax.numpy as jnp
from jax import lax
from jax.experimental import pallas as pl
from jax.experimental.pallas import tpu as pltpu
from jax.sharding import PartitionSpec as P

BLOCK = 128
PANEL = 32
SLAB = 8
MESH = pl.DeviceIdType.MESH
VMEM_LIMIT = 62 * 2**20
F32 = jnp.float32
BF16 = jnp.bfloat16


def split2(u):
    high = u.astype(BF16)
    return high, (u - high.astype(F32)).astype(BF16)


def split3(u):
    high = u.astype(BF16).astype(F32)
    rest = u - high
    mid = rest.astype(BF16).astype(F32)
    low = (rest - mid).astype(BF16).astype(F32)
    return high, mid, low


def inverse_factor(block):
    size = block.shape[0]
    slabs = PANEL // SLAB
    lane = lax.broadcasted_iota(jnp.int32, (SLAB, size), 1)
    row = lax.broadcasted_iota(jnp.int32, (SLAB, size), 0)
    below = block
    done = []
    for at in range(0, size, PANEL):
        top = [below[SLAB * t : SLAB * (t + 1)] for t in range(slabs)]
        columns = {}
        for c in range(PANEL):
            for t in range(c // SLAB, slabs):
                columns[c, t] = jnp.broadcast_to(top[t][:, at + c : at + c + 1], (SLAB, size))
        here = (lane >= at) & (lane < at + PANEL)
        body = [
            jnp.where(here, (lane - at == row + SLAB * t).astype(F32), top[t])
            for t in range(slabs)
        ]
        for j in range(PANEL):
            own, line = j // SLAB, j % SLAB
            root = lax.rsqrt(
                jnp.broadcast_to(columns[j, own][line : line + 1], (SLAB, size))
            )
            scaled = body[own][line : line + 1] * root
            factor = {t: columns[j, t] * root for t in range(own, slabs)}
            for c in range(j + 1, PANEL):
                there = c // SLAB
                across = jnp.broadcast_to(
                    factor[there][c % SLAB : c % SLAB + 1], (SLAB, size)
                )
                for t in range(there, slabs):
                    columns[c, t] = columns[c, t] - factor[t] * across
            under = jnp.where(row > line, factor[own], 0.0)
            body[own] = jnp.where(row == line, scaled, body[own] - under * scaled)
            for t in range(own + 1, slabs):
                body[t] = body[t] - factor[t] * scaled
        whole = jnp.concatenate(body, axis=0)
        done.append(whole)
        if at + PANEL < size:
            high, mid, low = split3(whole)
            left = jnp.concatenate([high, high, mid, high, mid, low], axis=0)
            right = jnp.concatenate([high, mid, high, low, mid, high], axis=0)
            outer = jnp.dot(
                left.T.astype(BF16)[at + PANEL :],
                right.astype(BF16),
                preferred_element_type=F32,
            )
            lanes = lax.broadcasted_iota(jnp.int32, outer.shape, 1)
            kept = jnp.where((lanes >= at) & (lanes < at + PANEL), 0.0, below[PANEL:])
            below = kept - outer
    whole = jnp.concatenate(done, axis=0)
    r = lax.broadcasted_iota(jnp.int32, (size, size), 0)
    c = lax.broadcasted_iota(jnp.int32, (size, size), 1)
    return jnp.where(c <= r, whole, 0.0)


def band(i):
    return slice(i * BLOCK, (i + 1) * BLOCK)


def eliminate(work, k):
    order = work.shape[0]
    blocks = order // BLOCK
    inverse = inverse_factor(work[band(k), band(k)])
    high, low = split2(inverse)
    parts = []
    if k > 0:
        parts.append(work[band(k), : k * BLOCK])
    if k + 1 < blocks:
        parts.append(work[band(k), (k + 1) * BLOCK :])
    rest_high, rest_low = split2(jnp.concatenate(parts, axis=1))
    product = jnp.dot(
        jnp.concatenate([high, high, low], axis=1),
        jnp.concatenate([rest_high, rest_low, rest_high], axis=0),
        preferred_element_type=F32,
    )
    if k > 0:
        work[band(k), : k * BLOCK] = product[:, : k * BLOCK]
    if k + 1 < blocks:
        work[band(k), (k + 1) * BLOCK :] = product[:, k * BLOCK :]
    work[band(k), band(k)] = inverse
    if k + 1 == blocks:
        return
    high, low = split2(work[band(k), :])
    right = jnp.concatenate([high, low, high], axis=0)
    for i in range(k + 1, blocks):
        high, low = split2(work[band(k), band(i)].T)
        left = jnp.concatenate([high, high, low], axis=1)
        change = jnp.dot(left, right[:, : (k + 1) * BLOCK], preferred_element_type=F32)
        if k > 0:
            work[band(i), : k * BLOCK] -= change[:, : k * BLOCK]
        work[band(i), band(k)] = -change[:, k * BLOCK :]
        work[band(i), i * BLOCK :] -= jnp.dot(
            left, right[:, i * BLOCK :], preferred_element_type=F32
        )


def place(owners):
    me = lax.axis_index("ops")
    return me, me // 2, lax.rem(me, 2)


def send(src, dst, send_sem, recv_sem, target, axis="ops"):
    return pltpu.make_async_remote_copy(
        src_ref=src,
        dst_ref=dst,
        send_sem=send_sem,
        recv_sem=recv_sem,
        device_id={axis: target},
        device_id_type=MESH,
    )


def greet(owners, sectors):
    me, pair, side = place(owners)
    half = owners // 2
    here = lax.axis_index("sector")
    chip, core, chips = here // 2, lax.rem(here, 2), sectors // 2
    barrier = pltpu.get_barrier_semaphore()
    targets = [{"ops": pair * 2 + 1 - side}, {"sector": chip * 2 + 1 - core}]
    targets += [{"ops": lax.rem(pair + k, half) * 2 + side} for k in range(1, half)]
    targets += [{"sector": lax.rem(chip + k, chips) * 2 + core} for k in range(1, chips)]
    for target in targets:
        pl.semaphore_signal(barrier, inc=1, device_id=target, device_id_type=MESH)
    pl.semaphore_wait(barrier, half + chips)


def gather_start(owners, own, blocks, send_sem, recv_sem):
    me, pair, side = place(owners)
    half = owners // 2
    for k in range(1, half):
        target = lax.rem(pair + k, half) * 2 + side
        send(own, blocks.at[me], send_sem.at[k], recv_sem.at[me], target).start()
    send(own, blocks.at[me], send_sem.at[0], recv_sem.at[me], pair * 2 + 1 - side).start()


def gather_receive(owners, own, blocks, send_sem, recv_sem, source):
    me, pair, side = place(owners)
    send(own, blocks.at[source], send_sem.at[0], recv_sem.at[source], me).wait_recv()


def gather_pass_on(owners, k, own, blocks, send_sem, recv_sem):
    me, pair, side = place(owners)
    half = owners // 2
    source = lax.rem(pair - k + half, half) * 2 + side
    gather_receive(owners, own, blocks, send_sem, recv_sem, source)
    send(
        blocks.at[source],
        blocks.at[source],
        send_sem.at[half - 1 + k],
        recv_sem.at[source],
        pair * 2 + 1 - side,
    ).start()
    return source


def gather_partner(owners, k, own, blocks, send_sem, recv_sem):
    me, pair, side = place(owners)
    half = owners // 2
    source = lax.rem(pair - k + half, half) * 2 + 1 - side
    gather_receive(owners, own, blocks, send_sem, recv_sem, source)
    return source


def gather_finish(owners, own, blocks, send_sem, recv_sem):
    me, pair, side = place(owners)
    for k in range(owners - 1):
        send(own, blocks.at[me], send_sem.at[k], recv_sem.at[me], me).wait_send()


def step_kernel(
    owners,
    sectors,
    psi_ref,
    diag_ref,
    dim_ref,
    index_ref,
    table_ref,
    left_hbm,
    right_hbm,
    basis_ref,
    energy_ref,
    next_ref,
    left,
    right,
    psi_all,
    psi_live,
    turned,
    sums,
    pair_out,
    pair_in,
    cross_out,
    cross_in,
    number,
    own,
    columns,
    work,
    operator,
    o_pair_in,
    o_cross_out,
    o_cross_in,
    o_own,
    o_whole,
    basis,
    one_out,
    one_in,
    two_out,
    two_in,
    three_in,
    load_sem,
    a_send,
    a_recv,
    p_send,
    p_recv,
    c_send,
    c_recv,
    n_send,
    n_recv,
    x_send,
    x_recv,
    op_send,
    op_recv,
    oc_send,
    oc_recv,
    og_send,
    og_recv,
    s_send,
    s_recv,
):
    me, pair, side = place(owners)
    half = owners // 2
    partner = pair * 2 + 1 - side
    rows, order = psi_ref.shape
    pairs = left.shape[0]
    dim = dim_ref[0]
    coef = [table_ref[index_ref[0, p]] for p in range(pairs)]

    loads = [pltpu.make_async_copy(right_hbm.at[0], right, load_sem.at[0])]
    loads.append(pltpu.make_async_copy(left_hbm.at[0], left, load_sem.at[1]))
    for load in loads:
        load.start()
    greet(owners, sectors)
    gather = (owners, psi_ref, psi_all, a_send, a_recv)
    gather_start(*gather)

    lane = lax.broadcasted_iota(jnp.int32, (rows, order), 1)
    row = lax.broadcasted_iota(jnp.int32, (rows, order), 0)

    def masked(block, owner):
        return jnp.where((lane < dim) & (row + owner * rows < dim), block, jnp.zeros_like(block))

    def turn(block, owner):
        live = masked(block, owner)
        psi_live[owner] = live
        for p in range(pairs):
            turned[p, pl.ds(pl.multiple_of(owner * rows, rows), rows), :] = (
                coef[p]
                * lax.dot_general(
                    live, right[p], (((1,), (1,)), ((), ())), preferred_element_type=F32
                )
            ).astype(BF16)

    loads[0].wait()
    turn(psi_ref[...], me)
    loads[1].wait()

    def operate(i, carry):
        here = pl.ds(pl.multiple_of(i * rows, rows), rows)
        total = coef[0] * left[0, here, :].astype(F32)
        for p in range(1, pairs):
            total += coef[p] * left[p, here, :].astype(F32)
        operator[i] = total.astype(BF16)
        return carry

    lax.fori_loop(0, owners, operate, 0)

    def o_pairing(k):
        return send(
            operator.at[lax.rem(pair + k, half) * 2 + 1 - side],
            o_pair_in.at[k - 1],
            op_send.at[k - 1],
            op_recv.at[k - 1],
            partner,
        )

    def o_crossing(k):
        return send(
            o_cross_out.at[k - 1],
            o_cross_in.at[k - 1],
            oc_send.at[k - 1],
            oc_recv.at[k - 1],
            lax.rem(pair + k, half) * 2 + side,
        )

    def o_pair_sum(k):
        o_pairing(k).wait_recv()
        mine = operator[lax.rem(pair + k, half) * 2 + side]
        return mine.astype(F32) + o_pair_in[k - 1].astype(F32)

    def o_cross(k, carry):
        o_cross_out[k - 1] = o_pair_sum(k).astype(BF16)
        o_crossing(k).start()
        return carry

    def o_start(k, carry):
        o_pairing(k).start()
        return carry

    def arrive(k, carry):
        source = gather_pass_on(owners, k, *gather[1:])
        turn(psi_all[source], source)
        source = gather_partner(owners, k - 1, *gather[1:])
        turn(psi_all[source], source)
        return carry

    lax.fori_loop(1, half, arrive, 0)
    o_pairing(1).start()
    source = gather_partner(owners, half - 1, *gather[1:])
    turn(psi_all[source], source)

    def partial(k, numer):
        at = lax.rem(pair + k, half)
        here = pl.ds(pl.multiple_of(at * 2 * rows, 2 * rows), 2 * rows)
        total = jnp.dot(left[0, here, :], turned[0], preferred_element_type=F32)
        for p in range(1, pairs):
            total += jnp.dot(left[p, here, :], turned[p], preferred_element_type=F32)
        sums[k - 1] = total.reshape(2, rows, order)
        pair_out[k - 1] = sums[k - 1, 1 - side].astype(BF16)
        send(
            pair_out.at[k - 1],
            pair_in.at[k - 1],
            p_send.at[k - 1],
            p_recv.at[k - 1],
            partner,
        ).start()
        for j in range(2):
            product = psi_live[at * 2 + j].astype(F32) * sums[k - 1, j]
            numer = numer + jnp.sum(product.reshape(rows // 8, 8, order), axis=0)
        return numer

    numer = lax.fori_loop(1, half + 1, partial, jnp.zeros((8, order), F32))
    lax.fori_loop(2, half, o_start, 0)
    number[0] = jnp.full((8, 128), jnp.sum(numer), F32)
    send(number.at[0], number.at[1], n_send.at[0], n_recv.at[0], partner).start()

    def square(i, carry):
        live = psi_live[i].astype(F32)
        return carry + jnp.sum((live * live).reshape(rows // 8, 8, order), axis=0)

    denom = jnp.sum(lax.fori_loop(0, owners, square, jnp.zeros((8, order), F32)))

    send(number.at[0], number.at[1], n_send.at[0], n_recv.at[0], partner).wait_recv()
    number[2 + pair] = number[0] + number[1]
    for k in range(1, half):
        send(
            number.at[2 + pair],
            number.at[2 + pair],
            n_send.at[k],
            n_recv.at[1 + pair],
            lax.rem(pair + k, half) * 2 + side,
        ).start()

    def crossing(k):
        return send(
            cross_out.at[k - 1],
            cross_in.at[k - 1],
            c_send.at[k - 1],
            c_recv.at[k - 1],
            lax.rem(pair + k, half) * 2 + side,
        )

    def pairing(k):
        return send(
            pair_out.at[k - 1], pair_in.at[k - 1], p_send.at[k - 1], p_recv.at[k - 1], partner
        )

    def cross(k, carry):
        pairing(k).wait_recv()
        cross_out[k - 1] = (sums[k - 1, side] + pair_in[k - 1].astype(F32)).astype(BF16)
        crossing(k).start()
        return carry

    o_cross(1, 0)
    lax.fori_loop(1, half, cross, 0)
    for k in range(1, half):
        source = lax.rem(pair + k, half)
        send(
            number.at[2 + pair], number.at[2 + source], n_send.at[k], n_recv.at[1 + source], me
        ).wait_recv()
    energy = number[2]
    for i in range(1, half):
        energy = energy + number[2 + i]
    energy = energy / denom
    energy_ref[...] = energy
    energy = jnp.max(energy)

    pairing(half).wait_recv()
    total = sums[half - 1, side] + pair_in[half - 1].astype(F32)
    sums[half - 1, side] = total

    def take(k, carry):
        crossing(k).wait_recv()
        sums[half - 1, side] += cross_in[k - 1].astype(F32)
        return carry

    lax.fori_loop(1, half, take, 0)
    sigma = masked(sums[half - 1, side], me)
    psi = psi_live[me].astype(F32)
    own[...] = (psi + (sigma - energy * psi) / diag_ref[...]).astype(BF16)
    gather = (owners, own, columns, x_send, x_recv)
    gather_start(*gather)

    step = 256

    def square_up(block, first):
        for i in range(0, order, step):
            part = lax.dot_general(
                block[:, i : i + step],
                block[:, i:],
                (((0,), (0,)), ((), ())),
                preferred_element_type=F32,
            )
            if first:
                work[i : i + step, i:] = part
            else:
                work[i : i + step, i:] += part

    columns[me] = own[...]
    square_up(own[...], True)

    def meet(k, carry):
        one = gather_pass_on(owners, k, *gather[1:])
        two = gather_partner(owners, k - 1, *gather[1:])
        square_up(jnp.concatenate([columns[one], columns[two]], axis=0), False)
        return carry

    lax.fori_loop(1, half, meet, 0)
    o_pairing(half).start()
    lax.fori_loop(2, half, o_cross, 0)
    last = gather_partner(owners, half - 1, *gather[1:])
    square_up(columns[last], False)

    o_gather = (owners, o_own, o_whole, og_send, og_recv)

    def o_settle():
        sums[0, 0] = o_pair_sum(half)

        def take(k, carry):
            o_crossing(k).wait_recv()
            sums[0, 0] += o_cross_in[k - 1].astype(F32)
            return carry

        lax.fori_loop(1, half, take, 0)
        o_own[...] = sums[0, 0].astype(BF16)
        gather_start(*o_gather)
        o_whole[me] = o_own[...]

    def o_hand_on(k, carry):
        gather_pass_on(owners, k, *o_gather[1:])
        return carry

    blocks = order // BLOCK
    r = lax.broadcasted_iota(jnp.int32, (BLOCK, BLOCK), 0)
    c = lax.broadcasted_iota(jnp.int32, (BLOCK, BLOCK), 1)
    ridge = jnp.where(r == c, 0.001 * order, 0.0).astype(F32)
    for i in range(blocks):
        work[band(i), band(i)] += ridge
    across = (((1,), (1,)), ((), ()))
    root = order**0.5

    def part_of_basis(rows_of, lines, depth):
        inverse = work[lines, :depth]
        if depth > BLOCK:
            col = lax.broadcasted_iota(jnp.int32, inverse.shape, 1)
            row_at = lax.broadcasted_iota(jnp.int32, inverse.shape, 0) + rows_of
            inverse = jnp.where(col <= row_at, inverse, 0.0)
        high, low = split2(inverse)
        return high, low

    ready = {}
    for k in range(1, half):
        ready.setdefault(blocks // 2 + (k - 1) * (blocks // 2) // max(half - 1, 1), []).append(k)
    for k in range(blocks):
        eliminate(work, k)
        if k == blocks // 4:
            o_settle()
        for j in ready.get(k, []):
            o_hand_on(j, 0)
        if k % 2 == 1:
            depth = (k + 1) * BLOCK
            high, low = part_of_basis(depth - 2 * BLOCK, slice(depth - 2 * BLOCK, depth), depth)
            x = columns[...].reshape(order, order)[:, :depth]
            basis[:, depth - 2 * BLOCK : depth] = (
                (
                    lax.dot_general(x, high, across, preferred_element_type=F32)
                    + lax.dot_general(x, low, across, preferred_element_type=F32)
                )
                * root
            ).astype(BF16)

    first = pl.multiple_of(me * rows, rows)
    mine = pl.ds(first, rows)
    high, low = part_of_basis(first, mine, order)
    x = columns[...].reshape(order, order)
    lines = (
        (
            lax.dot_general(high, x, across, preferred_element_type=F32)
            + lax.dot_general(low, x, across, preferred_element_type=F32)
        )
        * root
    ).astype(BF16)

    def o_partner(k, carry):
        gather_partner(owners, k, *o_gather[1:])
        return carry

    lax.fori_loop(0, half, o_partner, 0)
    turned_lines = jnp.dot(
        lines, o_whole[...].reshape(order, order), preferred_element_type=F32
    ).astype(BF16)
    next_ref[...] = jnp.dot(turned_lines, basis[...], preferred_element_type=F32) / order
    basis_ref[...] = basis[mine, :]
    sum_sectors(sectors, next_ref, one_out, one_in, two_out, two_in, three_in, s_send, s_recv)

    gather_finish(*gather)
    gather_finish(owners, psi_ref, psi_all, a_send, a_recv)
    gather_finish(*o_gather)
    for k in range(1, half + 1):
        pairing(k).wait_send()
        o_pairing(k).wait_send()
    for k in range(1, half):
        crossing(k).wait_send()
        o_crossing(k).wait_send()
    for k in range(half):
        send(number.at[0], number.at[1], n_send.at[k], n_recv.at[0], partner).wait_send()


def sum_sectors(sectors, rows_ref, one_out, one_in, two_out, two_in, three_in, sem_send, sem_recv):
    me = lax.axis_index("sector")
    core = lax.rem(me, 2)
    chip = me // 2
    chips = sectors // 2
    partner = chip * 2 + 1 - core
    rows, order = rows_ref.shape
    part = rows // 2
    kept = pl.ds(pl.multiple_of(core * part, part), part)
    given = pl.ds(pl.multiple_of((1 - core) * part, part), part)
    one_out[...] = rows_ref[given, :].astype(BF16)
    first = send(one_out, one_in, sem_send.at[0], sem_recv.at[0], partner, "sector")
    first.start()
    first.wait_recv()
    two_out[...] = (rows_ref[kept, :] + one_in[...].astype(F32)).astype(BF16)
    for k in range(1, chips):
        send(
            two_out,
            two_in.at[chip],
            sem_send.at[k],
            sem_recv.at[1 + chip],
            lax.rem(chip + k, chips) * 2 + core,
            "sector",
        ).start()
    two_in[chip] = two_out[...]
    for k in range(1, chips):
        source = lax.rem(chip + k, chips)
        send(
            two_out, two_in.at[source], sem_send.at[k], sem_recv.at[1 + source], me, "sector"
        ).wait_recv()
    total = two_in[0].astype(F32)
    for i in range(1, chips):
        total = total + two_in[i].astype(F32)
    two_in[0] = total.astype(BF16)
    last = send(two_in.at[0], three_in, sem_send.at[chips], sem_recv.at[chips + 1], partner, "sector")
    last.start()
    rows_ref[kept, :] = two_in[0].astype(F32)
    last.wait_recv()
    rows_ref[given, :] = three_in[...].astype(F32)
    first.wait_send()
    for k in range(1, chips):
        send(
            two_out, two_in.at[chip], sem_send.at[k], sem_recv.at[1 + chip], me, "sector"
        ).wait_send()
    last.wait_send()


def step_stage(psi, diag, dim, left, right, index, table):
    owners = lax.axis_size("ops")
    sectors = lax.axis_size("sector")
    half, chips = owners // 2, sectors // 2
    rows, order = psi.shape
    pairs = left.shape[1]
    vmem = pl.BlockSpec(memory_space=pltpu.VMEM)
    smem = pl.BlockSpec(memory_space=pltpu.SMEM)
    hbm = pl.BlockSpec(memory_space=pl.ANY)

    def held(*shape):
        return pltpu.VMEM(shape, BF16)

    sems = (2, owners, owners, half, half, half, half, half, half + 1, owners, owners)
    sems += (half, half, half, half, owners, owners, chips + 1, chips + 2)
    return pl.pallas_call(
        functools.partial(step_kernel, owners, sectors),
        out_shape=(
            jax.ShapeDtypeStruct((rows, order), BF16),
            jax.ShapeDtypeStruct((8, 128), F32),
            jax.ShapeDtypeStruct((rows, order), F32),
        ),
        in_specs=[vmem, vmem, smem, smem, smem, hbm, hbm],
        out_specs=(vmem, vmem, vmem),
        scratch_shapes=[
            held(pairs, order, order),
            held(pairs, order, order),
            held(owners, rows, order),
            held(owners, rows, order),
            held(pairs, order, order),
            pltpu.VMEM((half, 2, rows, order), F32),
            held(half, rows, order),
            held(half, rows, order),
            held(half, rows, order),
            held(half, rows, order),
            pltpu.VMEM((2 + half, 8, 128), F32),
            held(rows, order),
            held(owners, rows, order),
            pltpu.VMEM((order, order), F32),
            held(owners, rows, order),
            held(half, rows, order),
            held(half, rows, order),
            held(half, rows, order),
            held(rows, order),
            held(owners, rows, order),
            held(order, order),
            held(rows // 2, order),
            held(rows // 2, order),
            held(rows // 2, order),
            held(chips, rows // 2, order),
            held(rows // 2, order),
        ]
        + [pltpu.SemaphoreType.DMA((n,)) for n in sems],
        compiler_params=pltpu.CompilerParams(
            collective_id=0, has_side_effects=True, vmem_limit_bytes=VMEM_LIMIT
        ),
        cost_estimate=pl.CostEstimate(
            flops=20 * order**3, bytes_accessed=20 * order**2, transcendentals=0
        ),
        name="step_stage",
    )(psi, diag, dim, index, table, left, right)


def shards(wavefunction, diag_scale, sector_dims, left_ops, right_ops, weight_index, weight_table):
    basis, energy, next_rows = step_stage(
        wavefunction[0],
        diag_scale[0],
        sector_dims,
        left_ops,
        right_ops,
        weight_index,
        weight_table,
    )
    return (basis[None], energy[0, :1], next_rows)


def solution(mesh):
    in_specs = (
        P("sector", "ops", None),
        P("sector", "ops", None),
        P("sector"),
        P("sector", "ops", None, None),
        P("sector", "ops", None, None),
        P("sector", "ops"),
        P(),
    )
    out_specs = (P("sector", "ops", None), P("sector"), P("ops", None))
    return jax.shard_map(shards, mesh=mesh, in_specs=in_specs, out_specs=out_specs, check_vma=False)
```

```python
import functools

import jax
import jax.numpy as jnp
from jax import lax
from jax.experimental import pallas as pl
from jax.experimental.pallas import tpu as pltpu
from jax.sharding import PartitionSpec as P

BLOCK = 128
PANEL = 32
SLAB = 8
CHUNKS = 2
MESH = pl.DeviceIdType.MESH
VMEM_LIMIT = 62 * 2**20
F32 = jnp.float32
BF16 = jnp.bfloat16


def split2(u):
    high = u.astype(BF16)
    return high, (u - high.astype(F32)).astype(BF16)


def split3(u):
    high = u.astype(BF16).astype(F32)
    rest = u - high
    mid = rest.astype(BF16).astype(F32)
    low = (rest - mid).astype(BF16).astype(F32)
    return high, mid, low


def inverse_factor(block):
    size = block.shape[0]
    slabs = PANEL // SLAB
    lane = lax.broadcasted_iota(jnp.int32, (SLAB, size), 1)
    row = lax.broadcasted_iota(jnp.int32, (SLAB, size), 0)
    below = block
    done = []
    for at in range(0, size, PANEL):
        top = [below[SLAB * t : SLAB * (t + 1)] for t in range(slabs)]
        columns = {}
        for c in range(PANEL):
            for t in range(c // SLAB, slabs):
                columns[c, t] = jnp.broadcast_to(top[t][:, at + c : at + c + 1], (SLAB, size))
        here = (lane >= at) & (lane < at + PANEL)
        body = [
            jnp.where(here, (lane - at == row + SLAB * t).astype(F32), top[t])
            for t in range(slabs)
        ]
        for j in range(PANEL):
            own, line = j // SLAB, j % SLAB
            root = lax.rsqrt(
                jnp.broadcast_to(columns[j, own][line : line + 1], (SLAB, size))
            )
            scaled = body[own][line : line + 1] * root
            factor = {t: columns[j, t] * root for t in range(own, slabs)}
            for c in range(j + 1, PANEL):
                there = c // SLAB
                across = jnp.broadcast_to(
                    factor[there][c % SLAB : c % SLAB + 1], (SLAB, size)
                )
                for t in range(there, slabs):
                    columns[c, t] = columns[c, t] - factor[t] * across
            under = jnp.where(row > line, factor[own], 0.0)
            body[own] = jnp.where(row == line, scaled, body[own] - under * scaled)
            for t in range(own + 1, slabs):
                body[t] = body[t] - factor[t] * scaled
        whole = jnp.concatenate(body, axis=0)
        done.append(whole)
        if at + PANEL < size:
            high, mid, low = split3(whole)
            left = jnp.concatenate([high, high, mid, high, mid, low], axis=0)
            right = jnp.concatenate([high, mid, high, low, mid, high], axis=0)
            outer = jnp.dot(
                left.T.astype(BF16)[at + PANEL :],
                right.astype(BF16),
                preferred_element_type=F32,
            )
            lanes = lax.broadcasted_iota(jnp.int32, outer.shape, 1)
            kept = jnp.where((lanes >= at) & (lanes < at + PANEL), 0.0, below[PANEL:])
            below = kept - outer
    whole = jnp.concatenate(done, axis=0)
    r = lax.broadcasted_iota(jnp.int32, (size, size), 0)
    c = lax.broadcasted_iota(jnp.int32, (size, size), 1)
    return jnp.where(c <= r, whole, 0.0)


def band(i):
    return slice(i * BLOCK, (i + 1) * BLOCK)


def eliminate(work, k):
    order = work.shape[0]
    blocks = order // BLOCK
    inverse = inverse_factor(work[band(k), band(k)])
    high, low = split2(inverse)
    parts = []
    if k > 0:
        parts.append(work[band(k), : k * BLOCK])
    if k + 1 < blocks:
        parts.append(work[band(k), (k + 1) * BLOCK :])
    rest_high, rest_low = split2(jnp.concatenate(parts, axis=1))
    product = jnp.dot(
        jnp.concatenate([high, high, low], axis=1),
        jnp.concatenate([rest_high, rest_low, rest_high], axis=0),
        preferred_element_type=F32,
    )
    if k > 0:
        work[band(k), : k * BLOCK] = product[:, : k * BLOCK]
    if k + 1 < blocks:
        work[band(k), (k + 1) * BLOCK :] = product[:, k * BLOCK :]
    work[band(k), band(k)] = inverse
    if k + 1 == blocks:
        return
    high, low = split2(work[band(k), :])
    right = jnp.concatenate([high, low, high], axis=0)
    for i in range(k + 1, blocks):
        high, low = split2(work[band(k), band(i)].T)
        left = jnp.concatenate([high, high, low], axis=1)
        change = jnp.dot(left, right[:, : (k + 1) * BLOCK], preferred_element_type=F32)
        if k > 0:
            work[band(i), : k * BLOCK] -= change[:, : k * BLOCK]
        work[band(i), band(k)] = -change[:, k * BLOCK :]
        work[band(i), i * BLOCK :] -= jnp.dot(
            left, right[:, i * BLOCK :], preferred_element_type=F32
        )


def place(owners):
    me = lax.axis_index("ops")
    return me, me // 2, lax.rem(me, 2)


def send(src, dst, send_sem, recv_sem, target, axis="ops"):
    return pltpu.make_async_remote_copy(
        src_ref=src,
        dst_ref=dst,
        send_sem=send_sem,
        recv_sem=recv_sem,
        device_id={axis: target},
        device_id_type=MESH,
    )


def greet(owners, sectors):
    me, pair, side = place(owners)
    half = owners // 2
    here = lax.axis_index("sector")
    chip, core, chips = here // 2, lax.rem(here, 2), sectors // 2
    barrier = pltpu.get_barrier_semaphore()
    targets = [{"ops": pair * 2 + 1 - side}, {"sector": chip * 2 + 1 - core}]
    targets += [{"ops": lax.rem(pair + k, half) * 2 + side} for k in range(1, half)]
    targets += [{"sector": lax.rem(chip + k, chips) * 2 + core} for k in range(1, chips)]
    for target in targets:
        pl.semaphore_signal(barrier, inc=1, device_id=target, device_id_type=MESH)
    pl.semaphore_wait(barrier, half + chips)


def piece(c, order):
    return pl.ds(c * (order // CHUNKS), order // CHUNKS)


def within(value, count):
    return (value >= 0) & (value < count)


def gather_line(owners, own, blocks, send_sem, recv_sem, visit, finish=False):
    me, pair, side = place(owners)
    half = owners // 2
    order = own.shape[1]

    def copy(source_pair, c, way, source=None):
        at = source_pair * 2 + side
        here = blocks.at[at, :, piece(c, order)] if source is None else source
        target = pair * 2 + 1 - side
        if way:
            target = (pair + (1 if way == 1 else -1)) * 2 + side
        return send(
            here,
            blocks.at[at, :, piece(c, order)],
            send_sem.at[(way * half + source_pair) * CHUNKS + c],
            recv_sem.at[at * CHUNKS + c],
            target,
        )

    def arrived(at, c):
        there = blocks.at[at, :, piece(c, order)]
        send(there, there, send_sem.at[0], recv_sem.at[at * CHUNKS + c], me).wait_recv()

    if finish:
        def left_over(p, carry):
            for c in range(CHUNKS):
                copy(p, c, 0).wait_send()

                @pl.when((p <= pair) & (pair < half - 1))
                def _():
                    copy(p, c, 1).wait_send()

                @pl.when((p >= pair) & (pair > 0))
                def _():
                    copy(p, c, 2).wait_send()

            return carry

        lax.fori_loop(0, half, left_over, 0)
        return

    for c in range(CHUNKS):
        mine = own.at[:, piece(c, order)]

        @pl.when(pair < half - 1)
        def _():
            copy(pair, c, 1, mine).start()

        @pl.when(pair > 0)
        def _():
            copy(pair, c, 2, mine).start()

        copy(pair, c, 0, mine).start()

    def hop(d):
        for c in range(CHUNKS):
            for way, source in ((1, pair - d), (2, pair + d)):

                @pl.when(within(source, half))
                def _():
                    arrived(source * 2 + side, c)

                    @pl.when(pair < half - 1 if way == 1 else pair > 0)
                    def _():
                        copy(source, c, way).start()

                    copy(source, c, 0).start()

    def take(d):
        def one(g, carry):
            source = pair + (2 * g - 1) * d

            @pl.when(within(source, half) & (d + g > 0))
            def _():
                for c in range(CHUNKS):
                    arrived(source * 2 + 1 - side, c)
                visit(source)

            return carry

        lax.fori_loop(0, 2, one, 0)

    def step(d, carry):
        hop(d)
        take(d - 1)
        return carry

    lax.fori_loop(1, half + 1, step, 0)


def turn_of(owners, j):
    me, pair, side = place(owners)
    half = owners // 2
    last = j // (half - 1)
    upper = (2 * pair) // half
    down = half - 2 - j + (2 * half - 2 - j - pair) // half
    up = j + (j - pair + half) // half
    return (down * (1 - upper) + up * upper) * (1 - last) + pair * last


def reduce_line(owners, produce, between, sums, pair_out, pair_in, line_out, line_in, sems, finish=False):
    me, pair, side = place(owners)
    half = owners // 2
    order = pair_out.shape[2]
    p_send, p_recv, l_send, l_recv = sems

    def pairing(p, c):
        return send(
            pair_out.at[p, :, piece(c, order)],
            pair_in.at[p, :, piece(c, order)],
            p_send.at[p * CHUNKS + c],
            p_recv.at[p * CHUNKS + c],
            pair * 2 + 1 - side,
        )

    def moving(p, c, way, target):
        return send(
            line_out.at[p, :, piece(c, order)],
            line_in.at[way, p, :, piece(c, order)],
            l_send.at[p * CHUNKS + c],
            l_recv.at[(way * half + p) * CHUNKS + c],
            target,
        )

    if finish:
        def left_over(p, carry):
            for c in range(CHUNKS):
                pairing(p, c).wait_send()

                @pl.when(p != pair)
                def _():
                    moving(p, c, 0, me).wait_send()

            return carry

        lax.fori_loop(0, half, left_over, 0)
        return

    def serve(p):
        produce(p)
        pair_out[p] = sums[p, 1 - side].astype(BF16)
        for c in range(CHUNKS):
            pairing(p, c).start()

    def first(j, carry):
        serve(turn_of(owners, j))
        return carry

    lax.fori_loop(0, half, first, 0)
    between()

    def add(p, c, value):
        sums[p, side, :, piece(c, order)] += value.astype(F32)

    def pass_on(j, carry):
        p = turn_of(owners, j)
        for c in range(CHUNKS):
            pairing(p, c).wait_recv()
            add(p, c, pair_in[p, :, piece(c, order)])
            for way in range(2):
                ahead = p > pair if way == 0 else p < pair
                behind = pair > 0 if way == 0 else pair < half - 1

                @pl.when(ahead & behind)
                def _():
                    moving(p, c, way, me).wait_recv()
                    add(p, c, line_in[way, p, :, piece(c, order)])

            line_out[p, :, piece(c, order)] = sums[p, side, :, piece(c, order)].astype(BF16)
            for way in range(2):

                @pl.when(p > pair if way == 0 else p < pair)
                def _():
                    target = (pair + 1 - 2 * way) * 2 + side
                    moving(p, c, way, target).start()

        return carry

    lax.fori_loop(0, half - 1, pass_on, 0)
    for c in range(CHUNKS):
        pairing(pair, c).wait_recv()
        add(pair, c, pair_in[pair, :, piece(c, order)])
        for way in range(2):

            @pl.when(pair > 0 if way == 0 else pair < half - 1)
            def _():
                moving(pair, c, way, me).wait_recv()
                add(pair, c, line_in[way, pair, :, piece(c, order)])


def step_kernel(
    owners,
    sectors,
    psi_ref,
    diag_ref,
    dim_ref,
    index_ref,
    table_ref,
    left_hbm,
    right_hbm,
    basis_ref,
    energy_ref,
    next_ref,
    left,
    right,
    psi_all,
    psi_live,
    turned,
    sums,
    pair_out,
    pair_in,
    line_out,
    line_in,
    number,
    own,
    columns,
    work,
    operator,
    basis,
    moved,
    core_out,
    core_in,
    core_sums,
    f_pair_out,
    f_pair_in,
    f_line_out,
    f_line_in,
    two_out,
    two_in,
    three_in,
    load_sem,
    a_send,
    a_recv,
    p_send,
    p_recv,
    l_send,
    l_recv,
    n_send,
    n_recv,
    x_send,
    x_recv,
    d_send,
    d_recv,
    fp_send,
    fp_recv,
    fl_send,
    fl_recv,
    s_send,
    s_recv,
):
    me, pair, side = place(owners)
    half = owners // 2
    partner = pair * 2 + 1 - side
    rows, order = psi_ref.shape
    part = rows // 2
    pairs = left.shape[0]
    dim = dim_ref[0]
    coef = [table_ref[index_ref[0, p]] for p in range(pairs)]
    here = lax.axis_index("sector")
    chip, core, chips = here // 2, lax.rem(here, 2), sectors // 2
    core_partner = chip * 2 + 1 - core

    loads = [pltpu.make_async_copy(right_hbm.at[0], right, load_sem.at[0])]
    loads.append(pltpu.make_async_copy(left_hbm.at[0], left, load_sem.at[1]))
    for load in loads:
        load.start()
    greet(owners, sectors)

    def masked(block, first):
        lane = lax.broadcasted_iota(jnp.int32, block.shape, 1)
        row = lax.broadcasted_iota(jnp.int32, block.shape, 0)
        return jnp.where((lane < dim) & (row + first < dim), block, jnp.zeros_like(block))

    def pair_rows(p):
        return pl.ds(pl.multiple_of(p * 2 * rows, 2 * rows), 2 * rows)

    def both(blocks, p):
        return blocks[pl.ds(p * 2, 2)].reshape(2 * rows, order)

    def turn(p):
        live = masked(both(psi_all, p), p * 2 * rows)
        psi_live[pair_rows(p), :] = live
        for i in range(pairs):
            turned[i, pair_rows(p), :] = (
                coef[i]
                * lax.dot_general(
                    live, right[i], (((1,), (1,)), ((), ())), preferred_element_type=F32
                )
            ).astype(BF16)

    psi_all[me] = psi_ref[...]
    loads[0].wait()
    gather_line(owners, psi_ref, psi_all, a_send, a_recv, turn)
    loads[1].wait()

    def partial(p):
        total = jnp.dot(left[0, pair_rows(p), :], turned[0], preferred_element_type=F32)
        for i in range(1, pairs):
            total += jnp.dot(left[i, pair_rows(p), :], turned[i], preferred_element_type=F32)
        sums[p] = total.reshape(2, rows, order)
        product = psi_live[pair_rows(p), :].astype(F32) * sums[p].reshape(2 * rows, order)
        number[0] += fold(product)

    def fold(values):
        tall = jnp.sum(values.reshape(values.shape[0] // 8, 8, order), axis=0)
        total = tall[:, :128]
        for i in range(128, order, 128):
            total = total + tall[:, i : i + 128]
        return total

    number[0] = jnp.zeros((8, 128), F32)
    denoms = []

    def numbers(k, slot, target):
        return send(
            number.at[slot], number.at[slot], n_send.at[k], n_recv.at[slot], target
        )

    def exchange():
        number[2 + me] = number[0]
        for k in range(1, half):
            numbers(k, 2 + me, lax.rem(pair + k, half) * 2 + side).start()
        numbers(0, 2 + me, partner).start()

        def square(i, carry):
            live = psi_live[pl.ds(pl.multiple_of(i * BLOCK, BLOCK), BLOCK), :].astype(F32)
            return carry + fold(live * live)

        denoms.append(
            jnp.sum(lax.fori_loop(0, order // BLOCK, square, jnp.zeros((8, 128), F32)))
        )

        def operate(i, carry):
            at = pl.ds(pl.multiple_of(i * BLOCK, BLOCK), BLOCK)
            total = coef[0] * left[0, at, :].astype(F32)
            for p in range(1, pairs):
                total += coef[p] * left[p, at, :].astype(F32)
            operator[at, :] = total.astype(BF16)
            work[at, :] = jnp.zeros((BLOCK, order), F32)
            return carry

        lax.fori_loop(0, order // BLOCK, operate, 0)
        for k in range(1, half):
            source = lax.rem(pair + k, half) * 2 + side
            numbers(0, 2 + source, me).wait_recv()
            numbers(half - 1 + k, 2 + source, partner).start()

    reduction = (sums, pair_out, pair_in, line_out, line_in, (p_send, p_recv, l_send, l_recv))
    reduce_line(owners, partial, exchange, *reduction)
    for k in range(half):
        numbers(0, 2 + lax.rem(pair + k, half) * 2 + 1 - side, me).wait_recv()
    energy = number[2]
    for i in range(1, owners):
        energy = energy + number[2 + i]
    energy = jnp.full((8, 128), jnp.sum(energy), F32) / denoms[0]
    energy_ref[...] = energy
    energy = jnp.max(energy)

    sigma = masked(sums[pair, side], me * rows)
    psi = psi_live[pl.ds(pl.multiple_of(me * rows, rows), rows), :].astype(F32)
    own[...] = (psi + (sigma - energy * psi) / diag_ref[...]).astype(BF16)
    columns[me] = own[...]

    step = 256

    def square_up(p):
        block = both(columns, p)
        for i in range(0, order, step):
            work[i : i + step, i:] += lax.dot_general(
                block[:, i : i + step],
                block[:, i:],
                (((0,), (0,)), ((), ())),
                preferred_element_type=F32,
            )

    gather_line(owners, own, columns, x_send, x_recv, square_up)

    blocks = order // BLOCK
    r = lax.broadcasted_iota(jnp.int32, (BLOCK, BLOCK), 0)
    c = lax.broadcasted_iota(jnp.int32, (BLOCK, BLOCK), 1)
    ridge = jnp.where(r == c, 0.001 * order, 0.0).astype(F32)
    for i in range(blocks):
        work[band(i), band(i)] += ridge
    across = (((1,), (1,)), ((), ()))
    root = order**0.5
    for k in range(blocks):
        eliminate(work, k)
        if k % 2 == 1:
            depth = (k + 1) * BLOCK
            lines = slice(depth - 2 * BLOCK, depth)
            inverse = work[lines, :depth]
            col = lax.broadcasted_iota(jnp.int32, inverse.shape, 1)
            row = lax.broadcasted_iota(jnp.int32, inverse.shape, 0) + depth - 2 * BLOCK
            high, low = split2(jnp.where(col <= row, inverse, 0.0))
            x = columns[...].reshape(order, order)[:, :depth]
            basis[:, lines] = (
                (
                    lax.dot_general(x, high, across, preferred_element_type=F32)
                    + lax.dot_general(x, low, across, preferred_element_type=F32)
                )
                * root
            ).astype(BF16)
            moved[:, lines] = jnp.dot(
                operator[...], basis[:, lines], preferred_element_type=F32
            ).astype(BF16)

    def swapping(p):
        return send(
            core_out.at[p],
            core_in.at[p],
            d_send.at[p],
            d_recv.at[p],
            core_partner,
            "sector",
        )

    for p in range(half):
        sums[p] = lax.dot_general(
            basis[:, p * 2 * rows : (p + 1) * 2 * rows],
            moved[...],
            (((0,), (0,)), ((), ())),
            preferred_element_type=F32,
        ).reshape(2, rows, order) * (1.0 / order)
        given = sums[p, :, pl.ds(pl.multiple_of((1 - core) * part, part), part), :]
        core_out[p] = given.astype(BF16)
        swapping(p).start()

    def halves(p):
        swapping(p).wait_recv()
        kept = sums[p, :, pl.ds(pl.multiple_of(core * part, part), part), :]
        core_sums[p] = kept + core_in[p].astype(F32)

    last = (
        core_sums,
        f_pair_out,
        f_pair_in,
        f_line_out,
        f_line_in,
        (fp_send, fp_recv, fl_send, fl_recv),
    )
    reduce_line(owners, halves, lambda: None, *last)
    basis_ref[...] = basis[pl.ds(pl.multiple_of(me * rows, rows), rows), :]
    sum_chips(
        chips, core_sums[pair, side], next_ref, two_out, two_in, three_in, s_send, s_recv
    )

    gather_line(owners, psi_ref, psi_all, a_send, a_recv, None, finish=True)
    gather_line(owners, own, columns, x_send, x_recv, None, finish=True)
    reduce_line(owners, None, None, *reduction, finish=True)
    reduce_line(owners, None, None, *last, finish=True)

    def swapped(p, carry):
        swapping(p).wait_send()
        return carry

    lax.fori_loop(0, half, swapped, 0)
    for k in range(owners - 1):
        numbers(k, 2 + me, me).wait_send()


def sum_chips(chips, mine, rows_ref, two_out, two_in, three_in, sem_send, sem_recv):
    here = lax.axis_index("sector")
    chip, core = here // 2, lax.rem(here, 2)
    partner = chip * 2 + 1 - core
    part = mine.shape[0]
    two_out[...] = mine.astype(BF16)
    for k in range(1, chips):
        send(
            two_out,
            two_in.at[chip],
            sem_send.at[k],
            sem_recv.at[1 + chip],
            lax.rem(chip + k, chips) * 2 + core,
            "sector",
        ).start()
    two_in[chip] = two_out[...]
    for k in range(1, chips):
        source = lax.rem(chip + k, chips)
        send(
            two_out, two_in.at[source], sem_send.at[k], sem_recv.at[1 + source], here, "sector"
        ).wait_recv()
    total = two_in[0].astype(F32)
    for i in range(1, chips):
        total = total + two_in[i].astype(F32)
    two_out_sum = total.astype(BF16)
    three_in[core] = two_out_sum
    last = send(
        three_in.at[core],
        three_in.at[core],
        sem_send.at[0],
        sem_recv.at[0],
        partner,
        "sector",
    )
    last.start()
    rows_ref[pl.ds(pl.multiple_of(core * part, part), part), :] = two_out_sum.astype(F32)
    other = send(
        three_in.at[1 - core],
        three_in.at[1 - core],
        sem_send.at[0],
        sem_recv.at[0],
        here,
        "sector",
    )
    other.wait_recv()
    rows_ref[pl.ds(pl.multiple_of((1 - core) * part, part), part), :] = three_in[1 - core].astype(
        F32
    )
    last.wait_send()
    for k in range(1, chips):
        send(
            two_out, two_in.at[chip], sem_send.at[k], sem_recv.at[1 + chip], here, "sector"
        ).wait_send()


def step_stage(psi, diag, dim, left, right, index, table):
    owners = lax.axis_size("ops")
    sectors = lax.axis_size("sector")
    half, chips = owners // 2, sectors // 2
    rows, order = psi.shape
    part = rows // 2
    pairs = left.shape[1]
    vmem = pl.BlockSpec(memory_space=pltpu.VMEM)
    smem = pl.BlockSpec(memory_space=pltpu.SMEM)
    hbm = pl.BlockSpec(memory_space=pl.ANY)

    def held(*shape):
        return pltpu.VMEM(shape, BF16)

    gather = (3 * half * CHUNKS, owners * CHUNKS)
    reduce = (half * CHUNKS, half * CHUNKS, half * CHUNKS, 2 * half * CHUNKS)
    sems = (2,) + gather + reduce + (owners, owners + 2) + gather + (half, half) + reduce
    sems += (chips, chips + 1)
    return pl.pallas_call(
        functools.partial(step_kernel, owners, sectors),
        out_shape=(
            jax.ShapeDtypeStruct((rows, order), BF16),
            jax.ShapeDtypeStruct((8, 128), F32),
            jax.ShapeDtypeStruct((rows, order), F32),
        ),
        in_specs=[vmem, vmem, smem, smem, smem, hbm, hbm],
        out_specs=(vmem, vmem, vmem),
        scratch_shapes=[
            held(pairs, order, order),
            held(pairs, order, order),
            held(owners, rows, order),
            held(order, order),
            held(pairs, order, order),
            pltpu.VMEM((half, 2, rows, order), F32),
            held(half, rows, order),
            held(half, rows, order),
            held(half, rows, order),
            held(2, half, rows, order),
            pltpu.VMEM((2 + owners, 8, 128), F32),
            held(rows, order),
            held(owners, rows, order),
            pltpu.VMEM((order, order), F32),
            held(order, order),
            held(order, order),
            held(order, order),
            held(half, 2, part, order),
            held(half, 2, part, order),
            pltpu.VMEM((half, 2, part, order), F32),
            held(half, part, order),
            held(half, part, order),
            held(half, part, order),
            held(2, half, part, order),
            held(part, order),
            held(chips, part, order),
            held(2, part, order),
        ]
        + [pltpu.SemaphoreType.DMA((n,)) for n in sems],
        compiler_params=pltpu.CompilerParams(
            collective_id=0, has_side_effects=True, vmem_limit_bytes=VMEM_LIMIT
        ),
        cost_estimate=pl.CostEstimate(
            flops=20 * order**3, bytes_accessed=20 * order**2, transcendentals=0
        ),
        name="step_stage",
    )(psi, diag, dim, index, table, left, right)


def shards(wavefunction, diag_scale, sector_dims, left_ops, right_ops, weight_index, weight_table):
    basis, energy, next_rows = step_stage(
        wavefunction[0],
        diag_scale[0],
        sector_dims,
        left_ops,
        right_ops,
        weight_index,
        weight_table,
    )
    return (basis[None], energy[0, :1], next_rows)


def solution(mesh):
    in_specs = (
        P("sector", "ops", None),
        P("sector", "ops", None),
        P("sector"),
        P("sector", "ops", None, None),
        P("sector", "ops", None, None),
        P("sector", "ops"),
        P(),
    )
    out_specs = (P("sector", "ops", None), P("sector"), P("ops", None))
    return jax.shard_map(shards, mesh=mesh, in_specs=in_specs, out_specs=out_specs, check_vma=False)
```

```python
import functools

import jax
import jax.numpy as jnp
from jax import lax
from jax.experimental import pallas as pl
from jax.experimental.pallas import tpu as pltpu
from jax.sharding import PartitionSpec as P

BLOCK = 128
PANEL = 32
SLAB = 8
CHUNKS = 2
MESH = pl.DeviceIdType.MESH
VMEM_LIMIT = 62 * 2**20
F32 = jnp.float32
BF16 = jnp.bfloat16


def split2(u):
    high = u.astype(BF16)
    return high, (u - high.astype(F32)).astype(BF16)


def inverse_factor(block):
    size = block.shape[0]
    slabs = PANEL // SLAB
    lane = lax.broadcasted_iota(jnp.int32, (SLAB, size), 1)
    row = lax.broadcasted_iota(jnp.int32, (SLAB, size), 0)
    below = block
    done = []
    for at in range(0, size, PANEL):
        top = [below[SLAB * t : SLAB * (t + 1)] for t in range(slabs)]
        columns = {}
        for c in range(PANEL):
            for t in range(c // SLAB, slabs):
                columns[c, t] = jnp.broadcast_to(top[t][:, at + c : at + c + 1], (SLAB, size))
        here = (lane >= at) & (lane < at + PANEL)
        body = [
            jnp.where(here, (lane - at == row + SLAB * t).astype(F32), top[t])
            for t in range(slabs)
        ]
        for j in range(PANEL):
            own, line = j // SLAB, j % SLAB
            root = lax.rsqrt(
                jnp.broadcast_to(columns[j, own][line : line + 1], (SLAB, size))
            )
            scaled = body[own][line : line + 1] * root
            factor = {t: columns[j, t] * root for t in range(own, slabs)}
            for c in range(j + 1, PANEL):
                there = c // SLAB
                across = jnp.broadcast_to(
                    factor[there][c % SLAB : c % SLAB + 1], (SLAB, size)
                )
                for t in range(there, slabs):
                    columns[c, t] = columns[c, t] - factor[t] * across
            under = jnp.where(row > line, factor[own], 0.0)
            body[own] = jnp.where(row == line, scaled, body[own] - under * scaled)
            for t in range(own + 1, slabs):
                body[t] = body[t] - factor[t] * scaled
        whole = jnp.concatenate(body, axis=0)
        done.append(whole)
        if at + PANEL < size:
            high = whole.astype(BF16).astype(F32)
            low = whole - high
            outer = jnp.dot(
                jnp.concatenate([high, high, low], axis=0).T.astype(BF16)[at + PANEL :],
                jnp.concatenate([high, low, high], axis=0).astype(BF16),
                preferred_element_type=F32,
            )
            lanes = lax.broadcasted_iota(jnp.int32, outer.shape, 1)
            kept = jnp.where((lanes >= at) & (lanes < at + PANEL), 0.0, below[PANEL:])
            below = kept - outer
    whole = jnp.concatenate(done, axis=0)
    r = lax.broadcasted_iota(jnp.int32, (size, size), 0)
    c = lax.broadcasted_iota(jnp.int32, (size, size), 1)
    return jnp.where(c <= r, whole, 0.0)


def band(i):
    return slice(i * BLOCK, (i + 1) * BLOCK)


def eliminate(work, k):
    order = work.shape[0]
    blocks = order // BLOCK
    inverse = inverse_factor(work[band(k), band(k)])
    high, low = split2(inverse)
    parts = []
    if k > 0:
        parts.append(work[band(k), : k * BLOCK])
    if k + 1 < blocks:
        parts.append(work[band(k), (k + 1) * BLOCK :])
    rest_high, rest_low = split2(jnp.concatenate(parts, axis=1))
    product = jnp.dot(
        jnp.concatenate([high, high, low], axis=1),
        jnp.concatenate([rest_high, rest_low, rest_high], axis=0),
        preferred_element_type=F32,
    )
    if k > 0:
        work[band(k), : k * BLOCK] = product[:, : k * BLOCK]
    if k + 1 < blocks:
        work[band(k), (k + 1) * BLOCK :] = product[:, k * BLOCK :]
    work[band(k), band(k)] = inverse
    if k + 1 == blocks:
        return
    high, low = split2(work[band(k), :])
    right = jnp.concatenate([high, low, high], axis=0)
    for i in range(k + 1, blocks):
        high, low = split2(work[band(k), band(i)].T)
        left = jnp.concatenate([high, high, low], axis=1)
        change = jnp.dot(left, right[:, : (k + 1) * BLOCK], preferred_element_type=F32)
        if k > 0:
            work[band(i), : k * BLOCK] -= change[:, : k * BLOCK]
        work[band(i), band(k)] = -change[:, k * BLOCK :]
        work[band(i), i * BLOCK :] -= jnp.dot(
            left, right[:, i * BLOCK :], preferred_element_type=F32
        )


def place(owners):
    me = lax.axis_index("ops")
    return me, me // 2, lax.rem(me, 2)


def send(src, dst, send_sem, recv_sem, target, axis="ops"):
    return pltpu.make_async_remote_copy(
        src_ref=src,
        dst_ref=dst,
        send_sem=send_sem,
        recv_sem=recv_sem,
        device_id={axis: target},
        device_id_type=MESH,
    )


def greet(owners, sectors):
    me, pair, side = place(owners)
    half = owners // 2
    here = lax.axis_index("sector")
    chip, core, chips = here // 2, lax.rem(here, 2), sectors // 2
    barrier = pltpu.get_barrier_semaphore()
    targets = [{"ops": pair * 2 + 1 - side}, {"sector": chip * 2 + 1 - core}]
    targets += [{"ops": lax.rem(pair + k, half) * 2 + side} for k in range(1, half)]
    targets += [{"sector": lax.rem(chip + k, chips) * 2 + core} for k in range(1, chips)]
    for target in targets:
        pl.semaphore_signal(barrier, inc=1, device_id=target, device_id_type=MESH)
    pl.semaphore_wait(barrier, half + chips)


def piece(c, order):
    return pl.ds(c * (order // CHUNKS), order // CHUNKS)


def within(value, count):
    return (value >= 0) & (value < count)


def gather_line(owners, own, blocks, send_sem, recv_sem, visit, finish=False):
    me, pair, side = place(owners)
    half = owners // 2
    order = own.shape[1]

    def copy(source_pair, c, way, source=None):
        at = source_pair * 2 + side
        here = blocks.at[at, :, piece(c, order)] if source is None else source
        target = pair * 2 + 1 - side
        if way:
            target = (pair + (1 if way == 1 else -1)) * 2 + side
        return send(
            here,
            blocks.at[at, :, piece(c, order)],
            send_sem.at[(way * half + source_pair) * CHUNKS + c],
            recv_sem.at[at * CHUNKS + c],
            target,
        )

    def arrived(at, c):
        there = blocks.at[at, :, piece(c, order)]
        send(there, there, send_sem.at[0], recv_sem.at[at * CHUNKS + c], me).wait_recv()

    if finish:
        def left_over(p, carry):
            for c in range(CHUNKS):
                copy(p, c, 0).wait_send()

                @pl.when((p <= pair) & (pair < half - 1))
                def _():
                    copy(p, c, 1).wait_send()

                @pl.when((p >= pair) & (pair > 0))
                def _():
                    copy(p, c, 2).wait_send()

            return carry

        lax.fori_loop(0, half, left_over, 0)
        return

    for c in range(CHUNKS):
        mine = own.at[:, piece(c, order)]

        @pl.when(pair < half - 1)
        def _():
            copy(pair, c, 1, mine).start()

        @pl.when(pair > 0)
        def _():
            copy(pair, c, 2, mine).start()

        copy(pair, c, 0, mine).start()

    def hop(d):
        for c in range(CHUNKS):
            for way, source in ((1, pair - d), (2, pair + d)):

                @pl.when(within(source, half))
                def _():
                    arrived(source * 2 + side, c)

                    @pl.when(pair < half - 1 if way == 1 else pair > 0)
                    def _():
                        copy(source, c, way).start()

                    copy(source, c, 0).start()

    def take(d):
        def one(g, carry):
            source = pair + (2 * g - 1) * d

            @pl.when(within(source, half) & (d + g > 0))
            def _():
                for c in range(CHUNKS):
                    arrived(source * 2 + 1 - side, c)
                visit(source)

            return carry

        lax.fori_loop(0, 2, one, 0)

    def step(d, carry):
        hop(d)
        take(d - 1)
        return carry

    lax.fori_loop(1, half + 1, step, 0)


def turn_of(owners, j):
    me, pair, side = place(owners)
    half = owners // 2
    last = j // (half - 1)
    upper = (2 * pair) // half
    down = half - 2 - j + (2 * half - 2 - j - pair) // half
    up = j + (j - pair + half) // half
    return (down * (1 - upper) + up * upper) * (1 - last) + pair * last


def reduce_line(owners, produce, between, sums, pair_out, pair_in, line_out, line_in, sems, finish=False):
    me, pair, side = place(owners)
    half = owners // 2
    order = pair_out.shape[2]
    p_send, p_recv, l_send, l_recv = sems

    def pairing(p, c):
        return send(
            pair_out.at[p, :, piece(c, order)],
            pair_in.at[p, :, piece(c, order)],
            p_send.at[p * CHUNKS + c],
            p_recv.at[p * CHUNKS + c],
            pair * 2 + 1 - side,
        )

    def moving(p, c, way, target):
        return send(
            line_out.at[p, :, piece(c, order)],
            line_in.at[way, p, :, piece(c, order)],
            l_send.at[p * CHUNKS + c],
            l_recv.at[(way * half + p) * CHUNKS + c],
            target,
        )

    if finish:
        def left_over(p, carry):
            for c in range(CHUNKS):
                pairing(p, c).wait_send()

                @pl.when(p != pair)
                def _():
                    moving(p, c, 0, me).wait_send()

            return carry

        lax.fori_loop(0, half, left_over, 0)
        return

    def serve(p):
        produce(p)
        pair_out[p] = sums[p, 1 - side].astype(BF16)
        for c in range(CHUNKS):
            pairing(p, c).start()

    def first(j, carry):
        serve(turn_of(owners, j))
        return carry

    lax.fori_loop(0, half, first, 0)
    between()

    def add(p, c, value):
        sums[p, side, :, piece(c, order)] += value.astype(F32)

    def pass_on(j, carry):
        p = turn_of(owners, j)
        for c in range(CHUNKS):
            pairing(p, c).wait_recv()
            add(p, c, pair_in[p, :, piece(c, order)])
            for way in range(2):
                ahead = p > pair if way == 0 else p < pair
                behind = pair > 0 if way == 0 else pair < half - 1

                @pl.when(ahead & behind)
                def _():
                    moving(p, c, way, me).wait_recv()
                    add(p, c, line_in[way, p, :, piece(c, order)])

            line_out[p, :, piece(c, order)] = sums[p, side, :, piece(c, order)].astype(BF16)
            for way in range(2):

                @pl.when(p > pair if way == 0 else p < pair)
                def _():
                    target = (pair + 1 - 2 * way) * 2 + side
                    moving(p, c, way, target).start()

        return carry

    lax.fori_loop(0, half - 1, pass_on, 0)
    for c in range(CHUNKS):
        pairing(pair, c).wait_recv()
        add(pair, c, pair_in[pair, :, piece(c, order)])
        for way in range(2):

            @pl.when(pair > 0 if way == 0 else pair < half - 1)
            def _():
                moving(pair, c, way, me).wait_recv()
                add(pair, c, line_in[way, pair, :, piece(c, order)])


def step_kernel(
    owners,
    sectors,
    psi_ref,
    diag_ref,
    dim_ref,
    index_ref,
    table_ref,
    left_hbm,
    right_hbm,
    basis_ref,
    energy_ref,
    next_ref,
    left,
    right,
    psi_all,
    psi_live,
    turned,
    sums,
    pair_out,
    pair_in,
    line_out,
    line_in,
    number,
    own,
    columns,
    work,
    operator,
    basis,
    moved,
    core_out,
    core_in,
    core_sums,
    f_pair_out,
    f_pair_in,
    f_line_out,
    f_line_in,
    two_out,
    two_in,
    three_in,
    load_sem,
    a_send,
    a_recv,
    p_send,
    p_recv,
    l_send,
    l_recv,
    n_send,
    n_recv,
    x_send,
    x_recv,
    d_send,
    d_recv,
    fp_send,
    fp_recv,
    fl_send,
    fl_recv,
    s_send,
    s_recv,
):
    me, pair, side = place(owners)
    half = owners // 2
    partner = pair * 2 + 1 - side
    rows, order = psi_ref.shape
    part = rows // 2
    pairs = left.shape[0]
    dim = dim_ref[0]
    coef = [table_ref[index_ref[0, p]] for p in range(pairs)]
    here = lax.axis_index("sector")
    chip, core, chips = here // 2, lax.rem(here, 2), sectors // 2
    core_partner = chip * 2 + 1 - core

    loads = [pltpu.make_async_copy(right_hbm.at[0], right, load_sem.at[0])]
    loads.append(pltpu.make_async_copy(left_hbm.at[0], left, load_sem.at[1]))
    for load in loads:
        load.start()
    greet(owners, sectors)

    def masked(block, first):
        lane = lax.broadcasted_iota(jnp.int32, block.shape, 1)
        row = lax.broadcasted_iota(jnp.int32, block.shape, 0)
        return jnp.where((lane < dim) & (row + first < dim), block, jnp.zeros_like(block))

    def pair_rows(p):
        return pl.ds(pl.multiple_of(p * 2 * rows, 2 * rows), 2 * rows)

    def both(blocks, p):
        return blocks[pl.ds(p * 2, 2)].reshape(2 * rows, order)

    def turn(p):
        live = masked(both(psi_all, p), p * 2 * rows)
        psi_live[pair_rows(p), :] = live
        for i in range(pairs):
            turned[i, pair_rows(p), :] = (
                coef[i]
                * lax.dot_general(
                    live, right[i], (((1,), (1,)), ((), ())), preferred_element_type=F32
                )
            ).astype(BF16)

    psi_all[me] = psi_ref[...]
    loads[0].wait()
    gather_line(owners, psi_ref, psi_all, a_send, a_recv, turn)
    loads[1].wait()

    def partial(p):
        total = jnp.dot(left[0, pair_rows(p), :], turned[0], preferred_element_type=F32)
        for i in range(1, pairs):
            total += jnp.dot(left[i, pair_rows(p), :], turned[i], preferred_element_type=F32)
        sums[p] = total.reshape(2, rows, order)
        product = psi_live[pair_rows(p), :].astype(F32) * sums[p].reshape(2 * rows, order)
        number[0] += fold(product)

    def fold(values):
        tall = jnp.sum(values.reshape(values.shape[0] // 8, 8, order), axis=0)
        total = tall[:, :128]
        for i in range(128, order, 128):
            total = total + tall[:, i : i + 128]
        return total

    number[0] = jnp.zeros((8, 128), F32)
    denoms = []

    def numbers(k, slot, target):
        return send(
            number.at[slot], number.at[slot], n_send.at[k], n_recv.at[slot], target
        )

    def exchange():
        number[2 + me] = number[0]
        for k in range(1, half):
            numbers(k, 2 + me, lax.rem(pair + k, half) * 2 + side).start()
        numbers(0, 2 + me, partner).start()

        def square(i, carry):
            live = psi_live[pl.ds(pl.multiple_of(i * BLOCK, BLOCK), BLOCK), :].astype(F32)
            return carry + fold(live * live)

        denoms.append(
            jnp.sum(lax.fori_loop(0, order // BLOCK, square, jnp.zeros((8, 128), F32)))
        )

        def operate(i, carry):
            at = pl.ds(pl.multiple_of(i * BLOCK, BLOCK), BLOCK)
            total = coef[0] * left[0, at, :].astype(F32)
            for p in range(1, pairs):
                total += coef[p] * left[p, at, :].astype(F32)
            operator[at, :] = total.astype(BF16)
            work[at, :] = jnp.zeros((BLOCK, order), F32)
            return carry

        lax.fori_loop(0, order // BLOCK, operate, 0)
        for k in range(1, half):
            source = lax.rem(pair + k, half) * 2 + side
            numbers(0, 2 + source, me).wait_recv()
            numbers(half - 1 + k, 2 + source, partner).start()

    reduction = (sums, pair_out, pair_in, line_out, line_in, (p_send, p_recv, l_send, l_recv))
    reduce_line(owners, partial, exchange, *reduction)
    for k in range(half):
        numbers(0, 2 + lax.rem(pair + k, half) * 2 + 1 - side, me).wait_recv()
    energy = number[2]
    for i in range(1, owners):
        energy = energy + number[2 + i]
    energy = jnp.full((8, 128), jnp.sum(energy), F32) / denoms[0]
    energy_ref[...] = energy
    energy = jnp.max(energy)

    sigma = masked(sums[pair, side], me * rows)
    psi = psi_live[pl.ds(pl.multiple_of(me * rows, rows), rows), :].astype(F32)
    own[...] = (psi + (sigma - energy * psi) / diag_ref[...]).astype(BF16)
    columns[me] = own[...]

    step = 256

    def square_up(p):
        block = both(columns, p)
        for i in range(0, order, step):
            work[i : i + step, i:] += lax.dot_general(
                block[:, i : i + step],
                block[:, i:],
                (((0,), (0,)), ((), ())),
                preferred_element_type=F32,
            )

    gather_line(owners, own, columns, x_send, x_recv, square_up)

    blocks = order // BLOCK
    r = lax.broadcasted_iota(jnp.int32, (BLOCK, BLOCK), 0)
    c = lax.broadcasted_iota(jnp.int32, (BLOCK, BLOCK), 1)
    ridge = jnp.where(r == c, 0.001 * order, 0.0).astype(F32)
    for i in range(blocks):
        work[band(i), band(i)] += ridge
    across = (((1,), (1,)), ((), ()))
    root = order**0.5
    for k in range(blocks):
        eliminate(work, k)
        if k % 2 == 1:
            depth = (k + 1) * BLOCK
            lines = slice(depth - 2 * BLOCK, depth)
            inverse = work[lines, :depth]
            col = lax.broadcasted_iota(jnp.int32, inverse.shape, 1)
            row = lax.broadcasted_iota(jnp.int32, inverse.shape, 0) + depth - 2 * BLOCK
            high, low = split2(jnp.where(col <= row, inverse, 0.0))
            x = columns[...].reshape(order, order)[:, :depth]
            basis[:, lines] = (
                lax.dot_general(
                    jnp.concatenate([x, x], axis=1),
                    jnp.concatenate([high, low], axis=1),
                    across,
                    preferred_element_type=F32,
                )
                * root
            ).astype(BF16)
            moved[:, lines] = jnp.dot(
                operator[...], basis[:, lines], preferred_element_type=F32
            ).astype(BF16)

    def swapping(p):
        return send(
            core_out.at[p],
            core_in.at[p],
            d_send.at[p],
            d_recv.at[p],
            core_partner,
            "sector",
        )

    width = 2 * rows

    def rotate(p, lines):
        sums[p] = lax.dot_general(
            lines, moved[...], (((0,), (0,)), ((), ())), preferred_element_type=F32
        ).reshape(2, rows, order) * (1.0 / order)
        given = sums[p, :, pl.ds(pl.multiple_of((1 - core) * part, part), part), :]
        core_out[p] = given.astype(BF16)
        swapping(p).start()

    if width % 128:
        for p in range(half):
            rotate(p, basis[:, p * width : (p + 1) * width])
    else:

        def rotate_in_turn(j, carry):
            p = turn_of(owners, j)
            rotate(p, basis[:, pl.ds(pl.multiple_of(p * width, width), width)])
            return carry

        lax.fori_loop(0, half, rotate_in_turn, 0)

    def halves(p):
        swapping(p).wait_recv()
        kept = sums[p, :, pl.ds(pl.multiple_of(core * part, part), part), :]
        core_sums[p] = kept + core_in[p].astype(F32)

    last = (
        core_sums,
        f_pair_out,
        f_pair_in,
        f_line_out,
        f_line_in,
        (fp_send, fp_recv, fl_send, fl_recv),
    )
    reduce_line(owners, halves, lambda: None, *last)
    basis_ref[...] = basis[pl.ds(pl.multiple_of(me * rows, rows), rows), :]
    sum_chips(
        chips, core_sums[pair, side], next_ref, two_out, two_in, three_in, s_send, s_recv
    )

    gather_line(owners, psi_ref, psi_all, a_send, a_recv, None, finish=True)
    gather_line(owners, own, columns, x_send, x_recv, None, finish=True)
    reduce_line(owners, None, None, *reduction, finish=True)
    reduce_line(owners, None, None, *last, finish=True)

    def swapped(p, carry):
        swapping(p).wait_send()
        return carry

    lax.fori_loop(0, half, swapped, 0)
    for k in range(owners - 1):
        numbers(k, 2 + me, me).wait_send()


def sum_chips(chips, mine, rows_ref, two_out, two_in, three_in, sem_send, sem_recv):
    here = lax.axis_index("sector")
    chip, core = here // 2, lax.rem(here, 2)
    partner = chip * 2 + 1 - core
    part = mine.shape[0]
    two_out[...] = mine.astype(BF16)
    for k in range(1, chips):
        send(
            two_out,
            two_in.at[chip],
            sem_send.at[k],
            sem_recv.at[1 + chip],
            lax.rem(chip + k, chips) * 2 + core,
            "sector",
        ).start()
    two_in[chip] = two_out[...]
    for k in range(1, chips):
        source = lax.rem(chip + k, chips)
        send(
            two_out, two_in.at[source], sem_send.at[k], sem_recv.at[1 + source], here, "sector"
        ).wait_recv()
    total = two_in[0].astype(F32)
    for i in range(1, chips):
        total = total + two_in[i].astype(F32)
    two_out_sum = total.astype(BF16)
    three_in[core] = two_out_sum
    last = send(
        three_in.at[core],
        three_in.at[core],
        sem_send.at[0],
        sem_recv.at[0],
        partner,
        "sector",
    )
    last.start()
    rows_ref[pl.ds(pl.multiple_of(core * part, part), part), :] = two_out_sum.astype(F32)
    other = send(
        three_in.at[1 - core],
        three_in.at[1 - core],
        sem_send.at[0],
        sem_recv.at[0],
        here,
        "sector",
    )
    other.wait_recv()
    rows_ref[pl.ds(pl.multiple_of((1 - core) * part, part), part), :] = three_in[1 - core].astype(
        F32
    )
    last.wait_send()
    for k in range(1, chips):
        send(
            two_out, two_in.at[chip], sem_send.at[k], sem_recv.at[1 + chip], here, "sector"
        ).wait_send()


def step_stage(psi, diag, dim, left, right, index, table):
    owners = lax.axis_size("ops")
    sectors = lax.axis_size("sector")
    half, chips = owners // 2, sectors // 2
    rows, order = psi.shape
    part = rows // 2
    pairs = left.shape[1]
    vmem = pl.BlockSpec(memory_space=pltpu.VMEM)
    smem = pl.BlockSpec(memory_space=pltpu.SMEM)
    hbm = pl.BlockSpec(memory_space=pl.ANY)

    def held(*shape):
        return pltpu.VMEM(shape, BF16)

    gather = (3 * half * CHUNKS, owners * CHUNKS)
    reduce = (half * CHUNKS, half * CHUNKS, half * CHUNKS, 2 * half * CHUNKS)
    sems = (2,) + gather + reduce + (owners, owners + 2) + gather + (half, half) + reduce
    sems += (chips, chips + 1)
    return pl.pallas_call(
        functools.partial(step_kernel, owners, sectors),
        out_shape=(
            jax.ShapeDtypeStruct((rows, order), BF16),
            jax.ShapeDtypeStruct((8, 128), F32),
            jax.ShapeDtypeStruct((rows, order), F32),
        ),
        in_specs=[vmem, vmem, smem, smem, smem, hbm, hbm],
        out_specs=(vmem, vmem, vmem),
        scratch_shapes=[
            held(pairs, order, order),
            held(pairs, order, order),
            held(owners, rows, order),
            held(order, order),
            held(pairs, order, order),
            pltpu.VMEM((half, 2, rows, order), F32),
            held(half, rows, order),
            held(half, rows, order),
            held(half, rows, order),
            held(2, half, rows, order),
            pltpu.VMEM((2 + owners, 8, 128), F32),
            held(rows, order),
            held(owners, rows, order),
            pltpu.VMEM((order, order), F32),
            held(order, order),
            held(order, order),
            held(order, order),
            held(half, 2, part, order),
            held(half, 2, part, order),
            pltpu.VMEM((half, 2, part, order), F32),
            held(half, part, order),
            held(half, part, order),
            held(half, part, order),
            held(2, half, part, order),
            held(part, order),
            held(chips, part, order),
            held(2, part, order),
        ]
        + [pltpu.SemaphoreType.DMA((n,)) for n in sems],
        compiler_params=pltpu.CompilerParams(
            collective_id=0, has_side_effects=True, vmem_limit_bytes=VMEM_LIMIT
        ),
        cost_estimate=pl.CostEstimate(
            flops=20 * order**3, bytes_accessed=20 * order**2, transcendentals=0
        ),
        name="step_stage",
    )(psi, diag, dim, index, table, left, right)


def results_kernel(basis_ref, energy_ref, next_ref, basis_out, energy_out, next_out, sem):
    copies = [pltpu.make_async_copy(basis_ref, basis_out.at[0], sem.at[0])]
    copies.append(pltpu.make_async_copy(next_ref, next_out, sem.at[1]))
    for copy in copies:
        copy.start()
    energy_out[0] = jnp.max(energy_ref[...])
    for copy in copies:
        copy.wait()


def place_results(basis, energy, next_rows):
    vmem = pl.BlockSpec(memory_space=pltpu.VMEM)
    hbm = pl.BlockSpec(memory_space=pl.ANY)
    return pl.pallas_call(
        results_kernel,
        out_shape=(
            jax.ShapeDtypeStruct((1,) + basis.shape, basis.dtype),
            jax.ShapeDtypeStruct((1,), F32),
            jax.ShapeDtypeStruct(next_rows.shape, F32),
        ),
        in_specs=[vmem, vmem, vmem],
        out_specs=(hbm, pl.BlockSpec(memory_space=pltpu.SMEM), hbm),
        scratch_shapes=[pltpu.SemaphoreType.DMA((2,))],
        name="place_results",
    )(basis, energy, next_rows)


def shards(wavefunction, diag_scale, sector_dims, left_ops, right_ops, weight_index, weight_table):
    basis, energy, next_rows = step_stage(
        wavefunction[0],
        diag_scale[0],
        sector_dims,
        left_ops,
        right_ops,
        weight_index,
        weight_table,
    )
    return place_results(basis, energy, next_rows)


def solution(mesh):
    in_specs = (
        P("sector", "ops", None),
        P("sector", "ops", None),
        P("sector"),
        P("sector", "ops", None, None),
        P("sector", "ops", None, None),
        P("sector", "ops"),
        P(),
    )
    out_specs = (P("sector", "ops", None), P("sector"), P("ops", None))
    return jax.shard_map(shards, mesh=mesh, in_specs=in_specs, out_specs=out_specs, check_vma=False)
```
